32 devices in a mesh: groups: 2 (over y), blk: 16 (over z, x, core).
Axes of the slice: x: 2, y: 2, z: 4, core: 2. Of those that a mesh axis runs over, the one named last changes fastest.
Arguments:
- queries: bfloat16 [2048, 2048], P(('groups', 'blk')), parts along dimension 0, may hold values from -48 to 48
- rotated_cache_keys: bfloat16 [16384, 256], P(('groups', 'blk')), parts along dimension 0, may hold values from -4 to 4
- stored_cache_values: bfloat16 [16384, 256], P(('groups', 'blk')), parts along dimension 0, may hold values from -5 to 5
- segment_new_keys: bfloat16 [2048, 256], P(('groups', 'blk')), parts along dimension 0, may hold values from -4 to 4
- segment_new_values: bfloat16 [2048, 256], P(('groups', 'blk')), parts along dimension 0, may hold values from -5 to 5
- block_ids: int32 [2048, 8], P(('groups', 'blk')), parts along dimension 0, may hold values from 0 to 15, all different within a row; in each aligned block of 64 rows (0 to 63, 64 to 127, ...) at most 40 rows name the same one
- residual_in: bfloat16 [2048, 1024], P(('groups', 'blk')), parts along dimension 0, may hold values from -3 to 3
- out_weight: bfloat16 [2048, 1024], replicated, may hold values from -1.5 to 1.5
- norm_gain: float32 [1024], replicated, may hold values from 0.25 to 1.75
- expert_ids: int32 [2048, 8], P(('groups', 'blk')), parts along dimension 0, may hold values from 0 to 15, all different within a row; in each aligned block of 64 rows (0 to 63, 64 to 127, ...) at most 48 rows name the same one
- gate_scores: float32 [2048, 8], P(('groups', 'blk')), parts along dimension 0, may hold values from 0.05 to 1
- w_gate: bfloat16 [16, 1024, 768], P('blk'), may hold values from -0.1875 to 0.1875
- w_up: bfloat16 [16, 1024, 768], P('blk'), may hold values from -0.1875 to 0.1875
- w_down: bfloat16 [16, 768, 1024], P('blk'), may hold values from -0.21875 to 0.21875
Outputs:
- layer_out: bfloat16 [2048, 1024], P(('groups', 'blk')), parts along dimension 0
The draws below stay inside these ranges and needn't reach their ends.
There are 2 independent parts, one for each index of `groups`. The reference program is written for one: setup_inputs(seed, part) draws one part's arguments, and reference() takes and returns one part's arrays. A program takes and returns all parts, laid end to end along the dimension named above; an argument that names none is the same for every part. Nothing has to cross between parts.
Inputs may be any that keep to these rules, and one draw needn't show every extreme that they name: `block_ids`: each row names 8 different blocks. Among the rows of one device no block is named more than 40 times, and in some devices' rows some block is named exactly 40 times. `expert_ids`: each row names 8 different experts. Among the rows of one device no expert is named more than 48 times, and in some devices' rows some expert is named exactly 48 times.
All inputs are finite; a program needn't handle non-finite values.
Results may differ from the reference program's by a relative error of at most 0.0095.
Values may be sent and summed in bfloat16 or wider, within the bound.
No kernel may reach another device: no remote copies, remote signals or barrier semaphores. Data moves between devices by JAX's collectives and lax.ppermute only.
A program may use at most 128 MiB of HBM per device.

```python
import math
import jax
import jax.numpy as jnp
import numpy as np
from jax import lax

D = 1024
QUERY_HEADS = 16
KEY_VALUE_HEADS = 2
HEAD_SIZE = 128
FF = 768
TOPB = 8
TOPE = 8
TOKENS_PER_SHARD = 64
BLOCK_TOKENS = 512
SEGMENT_TOKENS = 1024
EXPERTS = 16
CAP = 40
CAP_E = 48
N_BLK = 16


def paired_draw(key):
    base = jax.random.fold_in(key, 11)
    first, latter_portion = jax.random.split(base, 2)
    query_vals = jnp.clip(jax.random.normal(first, (SEGMENT_TOKENS, QUERY_HEADS * HEAD_SIZE), jnp.float32), -4.0, 4.0)
    key_value_pairs = jnp.clip(jax.random.normal(latter_portion, (SEGMENT_TOKENS, KEY_VALUE_HEADS * HEAD_SIZE), jnp.float32), -4.0, 4.0)
    return (query_vals, key_value_pairs)


def draw_queries(key, part):
    return paired_draw(key)[0].astype(jnp.bfloat16)


def draw_segment_new_keys(key, part):
    return paired_draw(key)[1].astype(jnp.bfloat16)


def steps_of(own_key, extent, shards, low, largest):
    def one(axis_at, blocks):
        steps = jax.random.uniform(jax.random.fold_in(jax.random.fold_in(own_key, 6), axis_at), (blocks,), jnp.float32, low / len(shards), largest / len(shards))
        return jnp.repeat(jnp.exp(steps), extent[axis_at] // blocks).reshape((-1,) + (1,) * (len(extent) - axis_at - 1))

    loudness = one(*shards[0])
    for cut in shards[1:]:
        loudness = loudness * one(*cut)
    return loudness


def assign_block(rng, own, number, rows, number_of, top, reach, lean):
    sequence = jax.random.permutation(rng, number_of)
    packed, usual = portions_of(number_of, rows * top, reach, lean, True), portions_of(number_of, rows * top, reach, lean, False)
    places = jnp.arange(number_of)

    def named(lengths, rotation):
        used = int((lengths > 0).sum())
        fixed = max(1, used // 4)
        moved = fixed + (places - fixed + rotation * (used - fixed)) % max(1, number_of - fixed)
        return jnp.zeros((number_of,), jnp.int32).at[sequence[jnp.where(places < fixed, places, moved)]].set(jnp.asarray(lengths, jnp.int32))

    lengths = jnp.where(number % 4 == 0, named(packed, number // 4), named(usual, number - number // 4 - 1))
    mixed = jax.random.permutation(jax.random.fold_in(own, 3), number_of)
    donor, taker = mixed[0:number_of // 2 * 2:2], mixed[1:number_of // 2 * 2:2]
    room = jnp.minimum(lengths[donor] - 1, reach - lengths[taker]) // 2
    room = jnp.where((donor == sequence[0]) | (taker == sequence[0]) | (lengths[taker] == 0), 0, jnp.maximum(room, 0))
    moved = jax.random.randint(jax.random.fold_in(own, 4), (number_of // 2,), 0, 1 << 20) % (room + 1)
    lengths = lengths.at[donor].add(-moved).at[taker].add(moved)
    items = jnp.searchsorted(jnp.cumsum(lengths), jnp.arange(rows * top), side="right").astype(jnp.int32)
    listing = items.reshape(top, rows).T
    listing = listing[jax.random.permutation(jax.random.fold_in(own, 1), rows)]
    rotation = jax.random.randint(jax.random.fold_in(own, 2), (rows, 1), 0, top)
    return jnp.take_along_axis(listing, (jnp.arange(top)[None, :] + rotation) % top, axis=1)


def portions_of(number_of, total, bound, lean, full):
    weights = [(1 << 20) // math.isqrt(standing ** lean) + 1 for standing in range(1, number_of + 1)]
    largest = bound if full else min(bound, max(-(-total // number_of), total * weights[0] // sum(weights)))
    least = 1 if total - largest >= number_of - 1 else 0
    counts, surplus = [largest] + [least] * (number_of - 1), total - largest - least * (number_of - 1)
    while surplus > 0:
        candidates = [i for i in range(1, number_of) if counts[i] < largest] or [i for i in range(1, number_of) if counts[i] < bound]
        whole, budget = sum([weights[i] for i in candidates]), surplus
        for i in candidates:
            extra = min(bound - counts[i], max(1, budget * weights[i] // whole), surplus)
            counts[i] = counts[i] + extra
            surplus = surplus - extra
    return np.array(counts)


def bell_draw(rng, dims, spread, most, pieces=(), held_as=jnp.bfloat16):
    factor_of = steps_of(rng, dims, pieces, -0.22, 0.18) if pieces else 1.0
    values = jax.random.normal(rng, dims, jnp.float32) * spread * factor_of
    return jnp.minimum(jnp.maximum(values, -most), most).astype(held_as)


def setup_inputs(seed: int = 0, part: int = 0) -> dict:
    splits = jax.random.split(jax.random.key(seed), 15)
    own_keys = jax.random.split(jax.random.fold_in(splits[14], part), 15)
    queries = draw_queries(jax.random.fold_in(jax.random.fold_in(splits[14], part), 71), part)
    rotated_cache_keys = bell_draw(own_keys[1], (N_BLK * BLOCK_TOKENS, KEY_VALUE_HEADS * HEAD_SIZE), 1.0, 4.0, ((0, 16),))
    stored_cache_values = bell_draw(own_keys[2], (N_BLK * BLOCK_TOKENS, KEY_VALUE_HEADS * HEAD_SIZE), 1.0, 5.0, ((0, 16),))
    segment_new_keys = draw_segment_new_keys(jax.random.fold_in(jax.random.fold_in(splits[14], part), 71), part)
    segment_new_values = bell_draw(own_keys[4], (SEGMENT_TOKENS, KEY_VALUE_HEADS * HEAD_SIZE), 1.0, 5.0, ((0, 16),))
    block_ids_keys = jax.random.split(jax.random.fold_in(own_keys[5], 1), SEGMENT_TOKENS // TOKENS_PER_SHARD)
    block_ids_turns = jax.random.permutation(jax.random.fold_in(own_keys[5], 3), SEGMENT_TOKENS // TOKENS_PER_SHARD)
    block_ids = jax.vmap(lambda own, number: assign_block(jax.random.fold_in(own_keys[5], 2), own, number, TOKENS_PER_SHARD, N_BLK, TOPB, CAP, 2))(block_ids_keys, block_ids_turns).reshape((SEGMENT_TOKENS, TOPB))
    residual_in = bell_draw(own_keys[6], (SEGMENT_TOKENS, D), 0.5, 3.0, ((0, 16),))
    out_weight = bell_draw(splits[7], (QUERY_HEADS * HEAD_SIZE, D), 16 ** -0.5, 1.5)
    norm_gain = jnp.clip(1.0 + 0.15 * jax.random.normal(splits[8], (D,), jnp.float32), 0.25, 1.75)
    expert_ids_keys = jax.random.split(jax.random.fold_in(own_keys[9], 1), SEGMENT_TOKENS // TOKENS_PER_SHARD)
    expert_ids_turns = jax.random.permutation(jax.random.fold_in(own_keys[9], 3), SEGMENT_TOKENS // TOKENS_PER_SHARD)
    expert_ids = jax.vmap(lambda own, number: assign_block(jax.random.fold_in(own_keys[9], 2), own, number, TOKENS_PER_SHARD, EXPERTS, TOPE, CAP_E, 2))(expert_ids_keys, expert_ids_turns).reshape((SEGMENT_TOKENS, TOPE))
    gate_scores = jnp.clip(jnp.exp(math.log(1.0) - 2.9957323 * jax.random.uniform(own_keys[10], (SEGMENT_TOKENS, TOPE), jnp.float32) ** steps_of(own_keys[10], (SEGMENT_TOKENS, TOPE), ((0, 16),), -0.2, 0.2)), 0.05, 1.0)
    w_gate = bell_draw(splits[11], (EXPERTS, D, FF), D ** -0.5, 0.1875, ((0, 16),))
    w_up = bell_draw(splits[12], (EXPERTS, D, FF), D ** -0.5, 0.1875, ((0, 16),))
    w_down = bell_draw(splits[13], (EXPERTS, FF, D), FF ** -0.5, 0.21875, ((0, 16),))
    return {"queries": queries, "rotated_cache_keys": rotated_cache_keys, "stored_cache_values": stored_cache_values, "segment_new_keys": segment_new_keys, "segment_new_values": segment_new_values, "block_ids": block_ids, "residual_in": residual_in, "out_weight": out_weight, "norm_gain": norm_gain, "expert_ids": expert_ids, "gate_scores": gate_scores, "w_gate": w_gate, "w_up": w_up, "w_down": w_down}


NORM_EPSILON = 1e-06

def settle(values):
    return lax.optimization_barrier(values.astype(jnp.bfloat16)).astype(jnp.float32)

def reference(queries, rotated_cache_keys, stored_cache_values, segment_new_keys, segment_new_values, block_ids, residual_in, out_weight, norm_gain, expert_ids, gate_scores, w_gate, w_up, w_down):
    queries_per_cluster = QUERY_HEADS // KEY_VALUE_HEADS
    score_scale = HEAD_SIZE ** (-0.5)
    blocked_keys = rotated_cache_keys.reshape(N_BLK, BLOCK_TOKENS, KEY_VALUE_HEADS, HEAD_SIZE)
    blocked_values = stored_cache_values.reshape(N_BLK, BLOCK_TOKENS, KEY_VALUE_HEADS, HEAD_SIZE)

    def local_segment(inputs):
        segment_queries, segment_keys, segment_values = inputs
        heads_of_queries = segment_queries.astype(jnp.float32).reshape(TOKENS_PER_SHARD, KEY_VALUE_HEADS, queries_per_cluster, HEAD_SIZE)
        heads_of_keys = segment_keys.astype(jnp.float32).reshape(TOKENS_PER_SHARD, KEY_VALUE_HEADS, HEAD_SIZE)
        heads_of_values = segment_values.astype(jnp.float32).reshape(TOKENS_PER_SHARD, KEY_VALUE_HEADS, HEAD_SIZE)
        scores = jnp.einsum('qhgd,khd->qhgk', heads_of_queries, heads_of_keys) * score_scale
        places = jnp.arange(TOKENS_PER_SHARD, dtype=jnp.int32)
        allowed = places[None, :] <= places[:, None]
        scores = jnp.where(allowed[:, None, None, :], scores, -jnp.inf)
        row_max = lax.optimization_barrier(jnp.max(scores, axis=-1))
        weights = jnp.exp(scores - row_max[..., None])
        row_total = lax.optimization_barrier(jnp.sum(weights, axis=-1))
        merged = jnp.einsum('qhgk,khd->qhgd', settle(weights), heads_of_values)
        return (row_max.reshape(TOKENS_PER_SHARD, QUERY_HEADS), row_total.reshape(TOKENS_PER_SHARD, QUERY_HEADS), merged.reshape(TOKENS_PER_SHARD, QUERY_HEADS, HEAD_SIZE))
    local_row_maximum, local_denominator, local_output = lax.map(local_segment, (queries.reshape(N_BLK, TOKENS_PER_SHARD, QUERY_HEADS * HEAD_SIZE), segment_new_keys.reshape(N_BLK, TOKENS_PER_SHARD, KEY_VALUE_HEADS * HEAD_SIZE), segment_new_values.reshape(N_BLK, TOKENS_PER_SHARD, KEY_VALUE_HEADS * HEAD_SIZE)))
    local_row_maximum = local_row_maximum.reshape(SEGMENT_TOKENS // 16, 16, QUERY_HEADS)
    local_denominator = local_denominator.reshape(SEGMENT_TOKENS // 16, 16, QUERY_HEADS)
    local_output = local_output.reshape(SEGMENT_TOKENS // 16, 16, QUERY_HEADS, HEAD_SIZE)

    def cache_part(inputs):
        shard_queries, part_ids, part_max, part_total, part_out = inputs
        heads_of_queries = shard_queries.astype(jnp.float32).reshape(16, KEY_VALUE_HEADS, queries_per_cluster, HEAD_SIZE)
        chosen_keys = blocked_keys[part_ids].astype(jnp.float32)
        chosen_values = blocked_values[part_ids].astype(jnp.float32)
        scores = jnp.einsum('rhgd,rjkhd->rjhgk', heads_of_queries, chosen_keys) * score_scale
        row_max = lax.optimization_barrier(jnp.max(scores, axis=-1))
        weights = jnp.exp(scores - row_max[..., None])
        row_total = lax.optimization_barrier(jnp.sum(weights, axis=-1))
        merged = settle(jnp.einsum('rjhgk,rjkhd->rjhgd', settle(weights), chosen_values))
        row_max = row_max.reshape(16, TOPB, QUERY_HEADS)
        row_total = row_total.reshape(16, TOPB, QUERY_HEADS)
        merged = merged.reshape(16, TOPB, QUERY_HEADS, HEAD_SIZE)
        ceiling = jnp.maximum(part_max, lax.optimization_barrier(jnp.max(row_max, axis=1)))
        own_scale = jnp.exp(part_max - ceiling)
        pair_scale = jnp.exp(row_max - ceiling[:, None, :])
        denominator = part_total * own_scale + lax.optimization_barrier(jnp.sum(row_total * pair_scale, axis=1))
        numerator = part_out * own_scale[:, :, None] + lax.optimization_barrier(jnp.sum(merged * pair_scale[:, :, :, None], axis=1))
        return (numerator / denominator[:, :, None]).reshape(16, QUERY_HEADS * HEAD_SIZE).astype(jnp.bfloat16)
    attention = lax.map(cache_part, (queries.reshape(SEGMENT_TOKENS // 16, 16, QUERY_HEADS * HEAD_SIZE), block_ids.astype(jnp.int32).reshape(SEGMENT_TOKENS // 16, 16, TOPB), local_row_maximum, local_denominator, local_output))
    attention = attention.reshape(SEGMENT_TOKENS, QUERY_HEADS * HEAD_SIZE)
    hidden_state = residual_in.astype(jnp.float32) + jnp.dot(attention, out_weight, preferred_element_type=jnp.float32)
    normed = (hidden_state * lax.rsqrt(lax.optimization_barrier(jnp.mean(hidden_state * hidden_state, axis=-1, keepdims=True)) + NORM_EPSILON) * norm_gain.astype(jnp.float32)).astype(jnp.bfloat16)
    flat_experts = expert_ids.reshape(-1).astype(jnp.int32)
    pair_total = SEGMENT_TOKENS * TOPE
    ordering = jnp.argsort(flat_experts, stable=True).astype(jnp.int32)
    loads = lax.optimization_barrier(jnp.sum((flat_experts[:, None] == jnp.arange(EXPERTS, dtype=jnp.int32)[None, :]).astype(jnp.int32), axis=0))
    starts = jnp.cumsum(loads) - loads
    mixing = (gate_scores / lax.optimization_barrier(jnp.sum(gate_scores, axis=1, keepdims=True))).reshape(-1)

    def one_expert(accum, inputs):
        gate_matrix, up_matrix, down_matrix, start_at, load_of = inputs
        places = jnp.arange(N_BLK * CAP_E, dtype=jnp.int32)
        picked = ordering[jnp.minimum(start_at + places, pair_total - 1)]
        token_of = (picked // TOPE).astype(jnp.int32)
        rows_in = normed[token_of]
        gate_part = jnp.dot(rows_in, gate_matrix, preferred_element_type=jnp.float32)
        up_part = jnp.dot(rows_in, up_matrix, preferred_element_type=jnp.float32)
        inner = (jax.nn.silu(gate_part) * up_part).astype(jnp.bfloat16)
        expert_out = settle(jnp.dot(inner, down_matrix, preferred_element_type=jnp.float32))
        weight_of = jnp.where(places < load_of, mixing[picked], jnp.zeros((), mixing.dtype))
        accum = accum.at[token_of].add(weight_of[:, None] * expert_out)
        return (accum, None)
    mixture, unused = lax.scan(one_expert, jnp.zeros((SEGMENT_TOKENS, D), jnp.float32), (w_gate, w_up, w_down, starts.astype(jnp.int32), loads.astype(jnp.int32)))
    return (hidden_state + mixture).astype(jnp.bfloat16)
```

```python
import jax
import jax.numpy as jnp
from jax import lax
from jax.experimental import pallas as pl
from jax.experimental.pallas import tpu as pltpu
from jax.sharding import PartitionSpec as P

QUERY_HEADS = 16
KEY_VALUE_HEADS = 2
HEAD_SIZE = 128
TOPB = 8
TOPE = 8


NORM_EPSILON = 1e-06


def partials(query_rows, key_rows, value_rows, causal):
    queries_per_cluster = QUERY_HEADS // KEY_VALUE_HEADS
    score_scale = HEAD_SIZE ** (-0.5)
    maxima = []
    totals = []
    outputs = []
    for head_cluster in range(KEY_VALUE_HEADS):
        offset = head_cluster * queries_per_cluster * HEAD_SIZE
        group_queries = query_rows[:, offset : offset + queries_per_cluster * HEAD_SIZE].reshape(
            -1, HEAD_SIZE
        )
        group_keys = key_rows[:, head_cluster * HEAD_SIZE : (head_cluster + 1) * HEAD_SIZE]
        group_values = value_rows[:, head_cluster * HEAD_SIZE : (head_cluster + 1) * HEAD_SIZE]
        scores = (
            lax.dot_general(
                group_queries,
                group_keys,
                (((1,), (1,)), ((), ())),
                preferred_element_type=jnp.float32,
            )
            * score_scale
        )
        if causal:
            owner_row = jnp.arange(group_queries.shape[0], dtype=jnp.int32) // queries_per_cluster
            key_place = jnp.arange(key_rows.shape[0], dtype=jnp.int32)
            scores = jnp.where(key_place[None, :] <= owner_row[:, None], scores, -jnp.inf)
        row_max = jnp.max(scores, axis=1)
        weights = jnp.exp(scores - row_max[:, None])
        maxima.append(row_max.reshape(-1, queries_per_cluster))
        totals.append(jnp.sum(weights, axis=1).reshape(-1, queries_per_cluster))
        mixed_rows = jnp.dot(
            weights.astype(jnp.bfloat16), group_values, preferred_element_type=jnp.float32
        )
        outputs.append(mixed_rows.reshape(-1, queries_per_cluster * HEAD_SIZE))
    return (
        jnp.concatenate(maxima, axis=1),
        jnp.concatenate(totals, axis=1),
        jnp.concatenate(outputs, axis=1),
    )


def bucket_slots(targets, capacity, parties):
    flat_targets = targets.reshape(-1)
    pair_count = flat_targets.shape[0]
    one_hot = (flat_targets[:, None] == jnp.arange(parties, dtype=jnp.int32)[None, :]).astype(
        jnp.int32
    )
    before = jnp.sum((jnp.cumsum(one_hot, axis=0) - one_hot) * one_hot, axis=1)
    slot_index = flat_targets * capacity + before
    filler = (
        jnp.full((parties * capacity,), pair_count, jnp.int32)
        .at[slot_index]
        .set(jnp.arange(pair_count, dtype=jnp.int32))
    )
    return (slot_index, filler)


def routed_body(
    queries,
    rotated_cache_keys,
    stored_cache_values,
    segment_new_keys,
    segment_new_values,
    block_ids,
    residual_in,
    out_weight,
    norm_gain,
    expert_ids,
    gate_scores,
    w_gate,
    w_up,
    w_down,
):
    parties = lax.axis_size("blk")
    tok_count = queries.shape[0]
    capacity = tok_count * TOPB * 5 // (4 * parties)
    expert_capacity = tok_count * TOPE * 3 // (2 * parties)
    owner_slots, slot_pair = bucket_slots(block_ids, capacity, parties)
    pair_count = tok_count * TOPB
    occupied = slot_pair < pair_count
    source_token = jnp.minimum(slot_pair, pair_count - 1) // TOPB
    outgoing = jnp.where(
        occupied[:, None], queries[source_token], jnp.zeros((), queries.dtype)
    ).reshape(parties, capacity, QUERY_HEADS * HEAD_SIZE)
    arrived = lax.all_to_all(outgoing, "blk", split_axis=0, concat_axis=0, tiled=True)
    senders, items, row_width = arrived.shape
    far_max, far_total, far_out = partials(
        arrived.reshape(senders * items, row_width), rotated_cache_keys, stored_cache_values, False
    )
    back_max = lax.all_to_all(
        far_max.reshape(senders, items, QUERY_HEADS), "blk", split_axis=0, concat_axis=0, tiled=True
    )
    back_total = lax.all_to_all(
        far_total.reshape(senders, items, QUERY_HEADS),
        "blk",
        split_axis=0,
        concat_axis=0,
        tiled=True,
    )
    back_out = lax.all_to_all(
        far_out.astype(jnp.bfloat16).reshape(senders, items, row_width),
        "blk",
        split_axis=0,
        concat_axis=0,
        tiled=True,
    )
    local_row_maximum, local_denominator, local_output = partials(
        queries, segment_new_keys, segment_new_values, True
    )
    pair_max = back_max.reshape(-1, QUERY_HEADS)[owner_slots].reshape(tok_count, TOPB, QUERY_HEADS)
    pair_total = back_total.reshape(-1, QUERY_HEADS)[owner_slots].reshape(
        tok_count, TOPB, QUERY_HEADS
    )
    pair_out = back_out.reshape(-1, QUERY_HEADS * HEAD_SIZE)[owner_slots].reshape(
        tok_count, TOPB, QUERY_HEADS, HEAD_SIZE
    )
    ceiling = jnp.maximum(local_row_maximum, jnp.max(pair_max, axis=1))
    own_scale = jnp.exp(local_row_maximum - ceiling)
    pair_scale = jnp.exp(pair_max - ceiling[:, None, :])
    denominator = local_denominator * own_scale + jnp.sum(pair_total * pair_scale, axis=1)
    numerator = local_output.reshape(tok_count, QUERY_HEADS, HEAD_SIZE) * own_scale[
        :, :, None
    ] + jnp.einsum("tjh,tjhd->thd", pair_scale, pair_out, preferred_element_type=jnp.float32)
    attention = (
        (numerator / denominator[:, :, None])
        .reshape(tok_count, QUERY_HEADS * HEAD_SIZE)
        .astype(jnp.bfloat16)
    )
    hidden_state = residual_in.astype(jnp.float32) + jnp.dot(
        attention, out_weight, preferred_element_type=jnp.float32
    )
    normed = (
        hidden_state
        * lax.rsqrt(jnp.mean(hidden_state * hidden_state, axis=-1, keepdims=True) + NORM_EPSILON)
        * norm_gain
    ).astype(jnp.bfloat16)
    expert_slots, expert_pair = bucket_slots(expert_ids, expert_capacity, parties)
    expert_pairs = tok_count * TOPE
    expert_used = expert_pair < expert_pairs
    expert_token = jnp.minimum(expert_pair, expert_pairs - 1) // TOPE
    dispatched = jnp.where(
        expert_used[:, None], normed[expert_token], jnp.zeros((), normed.dtype)
    ).reshape(parties, expert_capacity, normed.shape[1])
    arrived = lax.all_to_all(dispatched, "blk", split_axis=0, concat_axis=0, tiled=True)
    flat_rows = arrived.reshape(-1, arrived.shape[2])
    gate_part = jnp.dot(flat_rows, w_gate[0], preferred_element_type=jnp.float32)
    up_part = jnp.dot(flat_rows, w_up[0], preferred_element_type=jnp.float32)
    inner = (jax.nn.silu(gate_part) * up_part).astype(jnp.bfloat16)
    expert_out = (
        jnp.dot(inner, w_down[0], preferred_element_type=jnp.float32)
        .astype(jnp.bfloat16)
        .reshape(arrived.shape)
    )
    returned = lax.all_to_all(expert_out, "blk", split_axis=0, concat_axis=0, tiled=True)
    gathered_rows = returned.reshape(-1, normed.shape[1])[expert_slots].reshape(
        tok_count, TOPE, normed.shape[1]
    )
    mixing = gate_scores / jnp.sum(gate_scores, axis=1, keepdims=True)
    mixture = jnp.einsum("tk,tkd->td", mixing, gathered_rows, preferred_element_type=jnp.float32)
    return (hidden_state + mixture).astype(jnp.bfloat16)


CORES = 2
LOG2_E = 1.4426950408889634
UNSEEN = -1e20
SKIPPED = 1e30
LANES = 128


def grid_of(parties):
    chips = parties // CORES
    across = round(chips ** (1 / 3))
    while chips % across:
        across -= 1
    return (chips // across, across)


def gathers(mesh):
    return mesh.shape["blk"] <= 4 * TOPB and mesh.shape["blk"] % CORES == 0


def shift_pairs(deep, across, step_deep, step_across, step_core):
    return [
        (
            (z * across + x) * CORES + c,
            ((z + step_deep) % deep * across + (x + step_across) % across) * CORES
            + (c + step_core) % CORES,
        )
        for z in range(deep)
        for x in range(across)
        for c in range(CORES)
    ]


def own_kernel(q_ref, k_ref, v_ref, top_ref, total_ref, out_ref):
    tokens = k_ref.shape[0]
    heads_per_group = QUERY_HEADS // KEY_VALUE_HEADS
    factor = HEAD_SIZE ** (-0.5) * LOG2_E
    rows = lax.broadcasted_iota(jnp.int32, (tokens, tokens), 0)
    keys = lax.broadcasted_iota(jnp.int32, (tokens, tokens), 1)
    lane = lax.broadcasted_iota(jnp.int32, (tokens, LANES), 1)
    top = jnp.full((tokens, LANES), UNSEEN, jnp.float32)
    total = jnp.zeros((tokens, LANES), jnp.float32)
    for head in range(QUERY_HEADS):
        group = head // heads_per_group
        at = slice(head * HEAD_SIZE, (head + 1) * HEAD_SIZE)
        of = slice(group * HEAD_SIZE, (group + 1) * HEAD_SIZE)
        scores = lax.dot_general(
            q_ref[:tokens, at],
            k_ref[:, of],
            (((1,), (1,)), ((), ())),
            preferred_element_type=jnp.float32,
        )
        scores = jnp.where(keys <= rows, scores * factor, -SKIPPED)
        high = jnp.max(scores, axis=1, keepdims=True)
        weights = jnp.exp2(scores - high)
        top = jnp.where(lane == head, high, top)
        total = jnp.where(lane == head, jnp.sum(weights, axis=1, keepdims=True), total)
        out_ref[:tokens, at] = jnp.dot(
            weights.astype(jnp.bfloat16), v_ref[:, of], preferred_element_type=jnp.float32
        )
    top_ref[:tokens, :] = top
    total_ref[:tokens, :] = total
    top_ref[tokens:, :] = jnp.full((tokens, LANES), UNSEEN, jnp.float32)
    total_ref[tokens:, :] = jnp.zeros((tokens, LANES), jnp.float32)
    out_ref[tokens:, :] = jnp.zeros((tokens, QUERY_HEADS * HEAD_SIZE), jnp.float32)


def own_partial(queries, keys, values):
    tokens = keys.shape[0]
    return pl.pallas_call(
        own_kernel,
        out_shape=(
            jax.ShapeDtypeStruct((2 * tokens, LANES), jnp.float32),
            jax.ShapeDtypeStruct((2 * tokens, LANES), jnp.float32),
            jax.ShapeDtypeStruct((2 * tokens, QUERY_HEADS * HEAD_SIZE), jnp.float32),
        ),
        name="own_partial",
    )(queries, keys, values)


def block_kernel(columns, group_list, count, *refs):
    q_ref, chosen_ref, top_in, total_in, out_in = refs[:5]
    block_refs = refs[5 : 5 + count]
    top_ref, total_ref, out_ref = refs[5 + count :]
    tokens = q_ref.shape[0]
    heads_per_group = QUERY_HEADS // KEY_VALUE_HEADS
    factor = HEAD_SIZE ** (-0.5) * LOG2_E
    lane = lax.broadcasted_iota(jnp.int32, (tokens, LANES), 1)
    top_ref[...] = top_in[...]
    total_ref[...] = total_in[...]
    fresh = set()
    for column, group, block_ref in zip(columns, group_list, block_refs):
        chosen = chosen_ref[:, column : column + 1] > 0.5
        ones = jnp.ones((block_ref.shape[0], LANES), jnp.bfloat16)
        for inner in range(heads_per_group):
            head = group * heads_per_group + inner
            at = slice(head * HEAD_SIZE, (head + 1) * HEAD_SIZE)
            scores = (
                lax.dot_general(
                    q_ref[:, at],
                    block_ref[:, :HEAD_SIZE],
                    (((1,), (1,)), ((), ())),
                    preferred_element_type=jnp.float32,
                )
                * factor
            )
            before = top_ref[:, head : head + 1]
            high = jnp.max(scores, axis=1, keepdims=True)
            high = jnp.maximum(before, jnp.where(chosen, high, UNSEEN))
            weights = jnp.exp2(scores - jnp.where(chosen, high, SKIPPED)).astype(jnp.bfloat16)
            mixed = jnp.dot(
                weights,
                jnp.concatenate([block_ref[:, HEAD_SIZE:], ones], axis=1),
                preferred_element_type=jnp.float32,
            )
            fade = jnp.exp2(before - high)
            old = out_in[:, at] if head not in fresh else out_ref[:, at]
            fresh.add(head)
            out_ref[:, at] = old * fade + mixed[:, :HEAD_SIZE]
            here = lane == head
            total = total_ref[...]
            total_ref[...] = jnp.where(here, total * fade + mixed[:, HEAD_SIZE:], total)
            top_ref[...] = jnp.where(here, high, top_ref[...])


def add_blocks(queries, chosen, state, blocks, columns, group_list):
    top, total, out = state
    kernel = lambda *refs: block_kernel(columns, group_list, len(blocks), *refs)
    rows = queries.shape[0]
    work = 4 * rows * HEAD_SIZE * (QUERY_HEADS // KEY_VALUE_HEADS) * blocks[0].shape[0]
    return pl.pallas_call(
        kernel,
        out_shape=tuple(jax.ShapeDtypeStruct(a.shape, a.dtype) for a in state),
        input_output_aliases={2: 0, 3: 1, 4: 2},
        cost_estimate=pl.CostEstimate(
            flops=work * len(blocks),
            bytes_accessed=out.size * 8 + sum(b.size for b in blocks) * 2,
            transcendentals=0,
        ),
        name="add_blocks",
    )(queries, chosen, top, total, out, *blocks)


def gathered_body(
    queries,
    rotated_cache_keys,
    stored_cache_values,
    segment_new_keys,
    segment_new_values,
    block_ids,
    residual_in,
    out_weight,
    norm_gain,
    expert_ids,
    gate_scores,
    w_gate,
    w_up,
    w_down,
):
    parties = lax.axis_size("blk")
    deep, across = grid_of(parties)
    tokens = queries.shape[0]
    width = residual_in.shape[1]
    place = lax.axis_index("blk")
    my_deep = place // (across * CORES)
    my_across = place // CORES % across
    my_core = place % CORES

    def moved(array, step_deep, step_across, step_core=0):
        return lax.ppermute(
            array, "blk", shift_pairs(deep, across, step_deep, step_across, step_core)
        )

    spots = [(dz, dx) for dz in range(deep) for dx in range(across)]
    sources = [
        ((my_deep - dz) % deep * across + (my_across - dx) % across) * CORES + my_core
        for dz, dx in spots
    ]

    chunks = []
    for group in range(KEY_VALUE_HEADS):
        of = slice(group * HEAD_SIZE, (group + 1) * HEAD_SIZE)
        chunks.append(
            jnp.concatenate([rotated_cache_keys[:, of], stored_cache_values[:, of]], axis=1)
        )
    blocks = {}
    for dz in [0] + [d for k in range(1, deep // 2 + 1) for d in sorted({k, deep - k})]:
        for group in range(KEY_VALUE_HEADS):
            if dz == 0:
                column = chunks[group]
            elif dz <= deep // 2:
                column = moved(blocks[dz - 1, 0, group], 1, 0)
            else:
                column = moved(blocks[(dz + 1) % deep, 0, group], -1, 0)
            blocks[dz, 0, group] = column
            for dx in range(1, across):
                blocks[dz, dx, group] = moved(column, 0, dx)

    pair_queries = jnp.concatenate([queries, moved(queries, 0, 0, 1)], axis=0)
    pair_ids = jnp.concatenate([block_ids, moved(block_ids, 0, 0, 1)], axis=0)
    chosen = jnp.any(
        pair_ids[:, :, None] == jnp.stack(sources)[None, None, :], axis=1
    ).astype(jnp.float32)
    chosen = jnp.pad(chosen, ((0, 0), (0, -len(spots) % LANES)))

    gates = jnp.concatenate([w_gate, moved(w_gate, 0, 0, 1)], axis=0)
    ups = jnp.concatenate([w_up, moved(w_up, 0, 0, 1)], axis=0)
    downs = jnp.concatenate([w_down, moved(w_down, 0, 0, 1)], axis=0)

    state = own_partial(queries, segment_new_keys, segment_new_values)
    order = [0] + [d for k in range(1, deep // 2 + 1) for d in sorted({k, deep - k})]
    for dz in order:
        for dx in range(across):
            state = add_blocks(
                pair_queries,
                chosen,
                state,
                [blocks[dz, dx, g] for g in range(KEY_VALUE_HEADS)],
                [dz * across + dx] * KEY_VALUE_HEADS,
                list(range(KEY_VALUE_HEADS)),
            )
    top, total, out = state
    far = [moved(a[tokens:], 0, 0, 1) for a in (top, total, out.astype(jnp.bfloat16))]
    near_top, far_top = top[:tokens, :QUERY_HEADS], far[0][:, :QUERY_HEADS]
    ceiling = jnp.maximum(near_top, far_top)
    near_scale = jnp.exp2(near_top - ceiling)
    far_scale = jnp.exp2(far_top - ceiling)
    denominator = total[:tokens, :QUERY_HEADS] * near_scale + far[1][:, :QUERY_HEADS] * far_scale
    near_scale = jnp.repeat(near_scale / denominator, HEAD_SIZE, axis=1)
    far_scale = jnp.repeat(far_scale / denominator, HEAD_SIZE, axis=1)
    attention = (out[:tokens] * near_scale + far[2].astype(jnp.float32) * far_scale).astype(
        jnp.bfloat16
    )
    hidden_state = residual_in.astype(jnp.float32) + jnp.dot(
        attention, out_weight, preferred_element_type=jnp.float32
    )
    normed = (
        hidden_state
        * lax.rsqrt(jnp.mean(hidden_state * hidden_state, axis=-1, keepdims=True) + NORM_EPSILON)
        * norm_gain
    ).astype(jnp.bfloat16)

    mixing = gate_scores / jnp.sum(gate_scores, axis=1, keepdims=True)
    experts = jnp.arange(parties, dtype=jnp.int32)
    spread = jnp.sum(
        jnp.where(expert_ids[:, :, None] == experts[None, None, :], mixing[:, :, None], 0.0), axis=1
    )
    coarse = spread.astype(jnp.bfloat16)
    fine = (spread - coarse.astype(jnp.float32)).astype(jnp.bfloat16)
    extra = jnp.concatenate([coarse, fine], axis=1)
    extra = jnp.pad(extra, ((0, 0), (0, -extra.shape[1] % LANES)))
    packed = jnp.concatenate([normed, extra], axis=1)

    rows = {(0, 0): packed}
    for dz in range(1, deep):
        rows[dz, 0] = moved(packed, dz, 0)
    for dz in range(deep):
        for dx in range(1, across):
            rows[dz, dx] = moved(rows[dz, 0], 0, dx)
    partner = place + 1 - 2 * my_core

    def run_experts(block):
        inputs = block[:, :width]
        weights = block[:, width : width + parties].astype(jnp.float32) + block[
            :, width + parties : width + 2 * parties
        ].astype(jnp.float32)
        result = 0.0
        for slot, expert in enumerate((place, partner)):
            gate_part = jnp.dot(inputs, gates[slot], preferred_element_type=jnp.float32)
            up_part = jnp.dot(inputs, ups[slot], preferred_element_type=jnp.float32)
            inner = (jax.nn.silu(gate_part) * up_part).astype(jnp.bfloat16)
            expert_out = jnp.dot(inner, downs[slot], preferred_element_type=jnp.float32)
            weight = jnp.sum(jnp.where(experts[None, :] == expert, weights, 0.0), axis=1)
            result = result + weight[:, None] * expert_out
        return result

    everything = jnp.concatenate([rows[spot] for spot in spots], axis=0)
    outcome = run_experts(everything).reshape(len(spots), tokens, width)
    outcome = {spot: outcome[n] for n, spot in enumerate(spots)}
    mixture = 0.0
    for dz in range(deep):
        column = outcome[dz, 0]
        for dx in range(1, across):
            column = column + moved(
                outcome[dz, dx].astype(jnp.bfloat16), 0, -dx
            ).astype(jnp.float32)
        if dz:
            column = moved(column.astype(jnp.bfloat16), -dz, 0).astype(jnp.float32)
        mixture = mixture + column
    return (hidden_state + mixture).astype(jnp.bfloat16)


def solution(mesh):
    placed = (
        P(("groups", "blk"), None),
        P(("groups", "blk"), None),
        P(("groups", "blk"), None),
        P(("groups", "blk"), None),
        P(("groups", "blk"), None),
        P(("groups", "blk"), None),
        P(("groups", "blk"), None),
        P(),
        P(),
        P(("groups", "blk"), None),
        P(("groups", "blk"), None),
        P("blk", None, None),
        P("blk", None, None),
        P("blk", None, None),
    )
    body = gathered_body if gathers(mesh) else routed_body
    return jax.shard_map(
        body, mesh=mesh, in_specs=placed, out_specs=P(("groups", "blk"), None), check_vma=False
    )
```

```python
import jax
import jax.numpy as jnp
from jax import lax
from jax.experimental import pallas as pl
from jax.experimental.pallas import tpu as pltpu
from jax.sharding import PartitionSpec as P

QUERY_HEADS = 16
KEY_VALUE_HEADS = 2
HEAD_SIZE = 128
TOPB = 8
TOPE = 8


NORM_EPSILON = 1e-06


def partials(query_rows, key_rows, value_rows, causal):
    queries_per_cluster = QUERY_HEADS // KEY_VALUE_HEADS
    score_scale = HEAD_SIZE ** (-0.5)
    maxima = []
    totals = []
    outputs = []
    for head_cluster in range(KEY_VALUE_HEADS):
        offset = head_cluster * queries_per_cluster * HEAD_SIZE
        group_queries = query_rows[:, offset : offset + queries_per_cluster * HEAD_SIZE].reshape(
            -1, HEAD_SIZE
        )
        group_keys = key_rows[:, head_cluster * HEAD_SIZE : (head_cluster + 1) * HEAD_SIZE]
        group_values = value_rows[:, head_cluster * HEAD_SIZE : (head_cluster + 1) * HEAD_SIZE]
        scores = (
            lax.dot_general(
                group_queries,
                group_keys,
                (((1,), (1,)), ((), ())),
                preferred_element_type=jnp.float32,
            )
            * score_scale
        )
        if causal:
            owner_row = jnp.arange(group_queries.shape[0], dtype=jnp.int32) // queries_per_cluster
            key_place = jnp.arange(key_rows.shape[0], dtype=jnp.int32)
            scores = jnp.where(key_place[None, :] <= owner_row[:, None], scores, -jnp.inf)
        row_max = jnp.max(scores, axis=1)
        weights = jnp.exp(scores - row_max[:, None])
        maxima.append(row_max.reshape(-1, queries_per_cluster))
        totals.append(jnp.sum(weights, axis=1).reshape(-1, queries_per_cluster))
        mixed_rows = jnp.dot(
            weights.astype(jnp.bfloat16), group_values, preferred_element_type=jnp.float32
        )
        outputs.append(mixed_rows.reshape(-1, queries_per_cluster * HEAD_SIZE))
    return (
        jnp.concatenate(maxima, axis=1),
        jnp.concatenate(totals, axis=1),
        jnp.concatenate(outputs, axis=1),
    )


def bucket_slots(targets, capacity, parties):
    flat_targets = targets.reshape(-1)
    pair_count = flat_targets.shape[0]
    one_hot = (flat_targets[:, None] == jnp.arange(parties, dtype=jnp.int32)[None, :]).astype(
        jnp.int32
    )
    before = jnp.sum((jnp.cumsum(one_hot, axis=0) - one_hot) * one_hot, axis=1)
    slot_index = flat_targets * capacity + before
    filler = (
        jnp.full((parties * capacity,), pair_count, jnp.int32)
        .at[slot_index]
        .set(jnp.arange(pair_count, dtype=jnp.int32))
    )
    return (slot_index, filler)


def routed_body(
    queries,
    rotated_cache_keys,
    stored_cache_values,
    segment_new_keys,
    segment_new_values,
    block_ids,
    residual_in,
    out_weight,
    norm_gain,
    expert_ids,
    gate_scores,
    w_gate,
    w_up,
    w_down,
):
    parties = lax.axis_size("blk")
    tok_count = queries.shape[0]
    capacity = tok_count * TOPB * 5 // (4 * parties)
    expert_capacity = tok_count * TOPE * 3 // (2 * parties)
    owner_slots, slot_pair = bucket_slots(block_ids, capacity, parties)
    pair_count = tok_count * TOPB
    occupied = slot_pair < pair_count
    source_token = jnp.minimum(slot_pair, pair_count - 1) // TOPB
    outgoing = jnp.where(
        occupied[:, None], queries[source_token], jnp.zeros((), queries.dtype)
    ).reshape(parties, capacity, QUERY_HEADS * HEAD_SIZE)
    arrived = lax.all_to_all(outgoing, "blk", split_axis=0, concat_axis=0, tiled=True)
    senders, items, row_width = arrived.shape
    far_max, far_total, far_out = partials(
        arrived.reshape(senders * items, row_width), rotated_cache_keys, stored_cache_values, False
    )
    back_max = lax.all_to_all(
        far_max.reshape(senders, items, QUERY_HEADS), "blk", split_axis=0, concat_axis=0, tiled=True
    )
    back_total = lax.all_to_all(
        far_total.reshape(senders, items, QUERY_HEADS),
        "blk",
        split_axis=0,
        concat_axis=0,
        tiled=True,
    )
    back_out = lax.all_to_all(
        far_out.astype(jnp.bfloat16).reshape(senders, items, row_width),
        "blk",
        split_axis=0,
        concat_axis=0,
        tiled=True,
    )
    local_row_maximum, local_denominator, local_output = partials(
        queries, segment_new_keys, segment_new_values, True
    )
    pair_max = back_max.reshape(-1, QUERY_HEADS)[owner_slots].reshape(tok_count, TOPB, QUERY_HEADS)
    pair_total = back_total.reshape(-1, QUERY_HEADS)[owner_slots].reshape(
        tok_count, TOPB, QUERY_HEADS
    )
    pair_out = back_out.reshape(-1, QUERY_HEADS * HEAD_SIZE)[owner_slots].reshape(
        tok_count, TOPB, QUERY_HEADS, HEAD_SIZE
    )
    ceiling = jnp.maximum(local_row_maximum, jnp.max(pair_max, axis=1))
    own_scale = jnp.exp(local_row_maximum - ceiling)
    pair_scale = jnp.exp(pair_max - ceiling[:, None, :])
    denominator = local_denominator * own_scale + jnp.sum(pair_total * pair_scale, axis=1)
    numerator = local_output.reshape(tok_count, QUERY_HEADS, HEAD_SIZE) * own_scale[
        :, :, None
    ] + jnp.einsum("tjh,tjhd->thd", pair_scale, pair_out, preferred_element_type=jnp.float32)
    attention = (
        (numerator / denominator[:, :, None])
        .reshape(tok_count, QUERY_HEADS * HEAD_SIZE)
        .astype(jnp.bfloat16)
    )
    hidden_state = residual_in.astype(jnp.float32) + jnp.dot(
        attention, out_weight, preferred_element_type=jnp.float32
    )
    normed = (
        hidden_state
        * lax.rsqrt(jnp.mean(hidden_state * hidden_state, axis=-1, keepdims=True) + NORM_EPSILON)
        * norm_gain
    ).astype(jnp.bfloat16)
    expert_slots, expert_pair = bucket_slots(expert_ids, expert_capacity, parties)
    expert_pairs = tok_count * TOPE
    expert_used = expert_pair < expert_pairs
    expert_token = jnp.minimum(expert_pair, expert_pairs - 1) // TOPE
    dispatched = jnp.where(
        expert_used[:, None], normed[expert_token], jnp.zeros((), normed.dtype)
    ).reshape(parties, expert_capacity, normed.shape[1])
    arrived = lax.all_to_all(dispatched, "blk", split_axis=0, concat_axis=0, tiled=True)
    flat_rows = arrived.reshape(-1, arrived.shape[2])
    gate_part = jnp.dot(flat_rows, w_gate[0], preferred_element_type=jnp.float32)
    up_part = jnp.dot(flat_rows, w_up[0], preferred_element_type=jnp.float32)
    inner = (jax.nn.silu(gate_part) * up_part).astype(jnp.bfloat16)
    expert_out = (
        jnp.dot(inner, w_down[0], preferred_element_type=jnp.float32)
        .astype(jnp.bfloat16)
        .reshape(arrived.shape)
    )
    returned = lax.all_to_all(expert_out, "blk", split_axis=0, concat_axis=0, tiled=True)
    gathered_rows = returned.reshape(-1, normed.shape[1])[expert_slots].reshape(
        tok_count, TOPE, normed.shape[1]
    )
    mixing = gate_scores / jnp.sum(gate_scores, axis=1, keepdims=True)
    mixture = jnp.einsum("tk,tkd->td", mixing, gathered_rows, preferred_element_type=jnp.float32)
    return (hidden_state + mixture).astype(jnp.bfloat16)


CORES = 2
LOG2_E = 1.4426950408889634
UNSEEN = -1e20
SKIPPED = 1e30
LANES = 128
TILE = 256
ONES_ROWS = 16


def grid_of(parties):
    chips = parties // CORES
    across = round(chips ** (1 / 3))
    while chips % across:
        across -= 1
    return (chips // across, across)


def gathers(mesh):
    return mesh.shape["blk"] <= 4 * TOPB and mesh.shape["blk"] % CORES == 0


def shift_pairs(deep, across, step_deep, step_across, step_core):
    return [
        (
            (z * across + x) * CORES + c,
            ((z + step_deep) % deep * across + (x + step_across) % across) * CORES
            + (c + step_core) % CORES,
        )
        for z in range(deep)
        for x in range(across)
        for c in range(CORES)
    ]


def attention_kernel(pieces, first, count, *refs):
    queries = refs[0:2]
    chosen_ref = refs[2]
    given = None if first else refs[3:7]
    block_refs = refs[-4 - count : -4]
    stats_refs = refs[-4:-2]
    out_refs = refs[-2:]
    tokens = queries[0].shape[0]
    per_tile = TILE // tokens
    heads_per_group = QUERY_HEADS // KEY_VALUE_HEADS
    factor = HEAD_SIZE ** (-0.5) * LOG2_E
    for group in range(KEY_VALUE_HEADS):
        mine = []
        for (of_group, column), block_ref in zip(pieces, block_refs):
            if of_group == group:
                values = block_ref[:, HEAD_SIZE:].astype(jnp.float32).T.astype(jnp.bfloat16)
                ones = jnp.ones((ONES_ROWS, values.shape[1]), jnp.bfloat16)
                mine.append((column, block_ref, jnp.concatenate([values, ones], axis=0)))
        for owner in range(2):
            for tile in range(heads_per_group // per_tile):
                head = group * heads_per_group + tile * per_tile
                at = slice(head * tokens, head * tokens + TILE)
                rows = jnp.concatenate(
                    [
                        queries[owner][:, h * HEAD_SIZE : (h + 1) * HEAD_SIZE]
                        for h in range(head, head + per_tile)
                    ],
                    axis=0,
                )
                if first:
                    top = jnp.full((1, TILE), UNSEEN, jnp.float32)
                    total = jnp.zeros((1, TILE), jnp.float32)
                    out = jnp.zeros((HEAD_SIZE, TILE), jnp.float32)
                else:
                    top = given[owner][0:1, at]
                    total = given[owner][1:2, at]
                    out = given[2 + owner][:, at].astype(jnp.float32)
                for column, block_ref, mixer in mine:
                    if column is None and owner:
                        continue
                    scores = lax.dot_general(
                        block_ref[:, :HEAD_SIZE],
                        rows,
                        (((1,), (1,)), ((), ())),
                        preferred_element_type=jnp.float32,
                    )
                    if column is None:
                        key = lax.broadcasted_iota(jnp.int32, scores.shape, 0)
                        token = lax.broadcasted_iota(jnp.int32, scores.shape, 1) % tokens
                        scores = jnp.where(key <= token, scores, -SKIPPED)
                        high = jnp.maximum(top, jnp.max(scores, axis=0, keepdims=True) * factor)
                        shift = high
                    else:
                        chosen = chosen_ref[
                            column : column + 1, owner * TILE : (owner + 1) * TILE
                        ]
                        high = jnp.max(scores, axis=0, keepdims=True) * factor
                        high = jnp.maximum(top, jnp.where(chosen > 0.5, high, UNSEEN))
                        shift = jnp.where(chosen > 0.5, high, SKIPPED)
                    weights = jnp.exp2(scores * factor - shift).astype(jnp.bfloat16)
                    mixed = jnp.dot(mixer, weights, preferred_element_type=jnp.float32)
                    fade = jnp.exp2(top - high)
                    out = out * fade + mixed[:HEAD_SIZE]
                    total = total * fade + mixed[HEAD_SIZE : HEAD_SIZE + 1]
                    top = high
                stats_refs[owner][0:1, at] = top
                stats_refs[owner][1:2, at] = total
                out_refs[owner][:, at] = out.astype(out_refs[owner].dtype)


def attend(queries, chosen, state, pieces, blocks, last=False):
    tokens = queries[0].shape[0]
    span = QUERY_HEADS * tokens
    stats = jax.ShapeDtypeStruct((8, span), jnp.float32)
    out = jax.ShapeDtypeStruct((HEAD_SIZE, span), jnp.float32)
    sent = jax.ShapeDtypeStruct((HEAD_SIZE, span), jnp.bfloat16)
    count = len(blocks)
    keys = sum(b.shape[0] for b in blocks)
    return pl.pallas_call(
        lambda *refs: attention_kernel(pieces, state is None, count, *refs),
        out_shape=(stats, stats, out, sent if last else out),
        cost_estimate=pl.CostEstimate(
            flops=4 * keys * span * HEAD_SIZE,
            bytes_accessed=16 * HEAD_SIZE * span + keys * HEAD_SIZE * 4,
            transcendentals=keys * span,
        ),
        name="attend_blocks",
    )(*queries, chosen, *(state or ()), *blocks)


def finish_kernel(
    near_stats,
    near_out,
    far_stats,
    far_out,
    weight_ref,
    residual_ref,
    gain_ref,
    extra_ref,
    hidden_ref,
    packed_ref,
):
    tokens, width = residual_ref.shape
    near_top, far_top = near_stats[0:1, :], far_stats[0:1, :]
    ceiling = jnp.maximum(near_top, far_top)
    near_scale = jnp.exp2(near_top - ceiling)
    far_scale = jnp.exp2(far_top - ceiling)
    total = near_stats[1:2, :] * near_scale + far_stats[1:2, :] * far_scale
    mixed = near_out[...] * (near_scale / total) + far_out[...].astype(jnp.float32) * (
        far_scale / total
    )
    per_turn = LANES // tokens
    heads = []
    for turn in range(QUERY_HEADS // per_turn):
        turned = mixed[:, turn * LANES : (turn + 1) * LANES].T.astype(jnp.bfloat16)
        heads.extend(turned[n * tokens : (n + 1) * tokens] for n in range(per_turn))
    attention = jnp.concatenate(heads, axis=1)
    hidden = residual_ref[...].astype(jnp.float32) + jnp.dot(
        attention, weight_ref[...], preferred_element_type=jnp.float32
    )
    hidden_ref[...] = hidden
    mean = jnp.mean(hidden * hidden, axis=-1, keepdims=True)
    packed_ref[:, :width] = (hidden * lax.rsqrt(mean + NORM_EPSILON) * gain_ref[...]).astype(
        jnp.bfloat16
    )
    packed_ref[:, width:] = extra_ref[...]


def expert_kernel(parties, rows_count, *refs):
    who_ref = refs[0]
    row_refs = refs[1 : 1 + rows_count]
    weight_refs = refs[1 + rows_count : 7 + rows_count]
    out_refs = refs[7 + rows_count : 7 + 2 * rows_count]
    (sum_ref,) = refs[7 + 2 * rows_count :]
    step = pl.program_id(0)
    tokens, width = out_refs[0].shape
    block = jnp.concatenate([r[...] for r in row_refs], axis=0)
    inputs = block[:, :width]
    extra = block[:, width:].astype(jnp.float32)
    lane = lax.broadcasted_iota(jnp.int32, extra.shape, 1)
    result = None
    for slot in range(2):
        gate_ref, up_ref, down_ref = weight_refs[3 * slot : 3 * slot + 3]
        expert = who_ref[slot]
        here = (lane == expert) | (lane == expert + parties)
        weight = jnp.sum(jnp.where(here, extra, 0.0), axis=1, keepdims=True)
        gate = jnp.dot(inputs, gate_ref[0], preferred_element_type=jnp.float32)
        up = jnp.dot(inputs, up_ref[0], preferred_element_type=jnp.float32)
        inner = (gate / (1.0 + jnp.exp(-gate)) * up).astype(jnp.bfloat16)
        part = weight * jnp.dot(inner, down_ref[0], preferred_element_type=jnp.float32)
        result = part if result is None else result + part

    @pl.when(step == 0)
    def _():
        sum_ref[...] = result

    @pl.when(step > 0)
    def _():
        sum_ref[...] += result

    @pl.when(step == pl.num_programs(0) - 1)
    def _():
        for n, out_ref in enumerate(out_refs):
            out_ref[...] = sum_ref[n * tokens : (n + 1) * tokens, :].astype(out_ref.dtype)


def run_experts(parties, who, rows, weights, out_types):
    tokens, packed_width = rows[0].shape
    width = weights[0].shape[1]
    hidden = weights[0].shape[2]
    step = 2 * LANES
    whole = pl.BlockSpec((tokens, packed_width), lambda f: (0, 0))
    out = pl.BlockSpec((tokens, width), lambda f: (0, 0))
    into = pl.BlockSpec((1, width, step), lambda f: (0, 0, f))
    back = pl.BlockSpec((1, step, width), lambda f: (0, f, 0))
    return pl.pallas_call(
        lambda *refs: expert_kernel(parties, len(rows), *refs),
        grid=(hidden // step,),
        in_specs=[pl.BlockSpec(memory_space=pltpu.SMEM)]
        + [whole] * len(rows)
        + [into, into, back] * 2,
        out_specs=[out] * len(rows),
        out_shape=[jax.ShapeDtypeStruct((tokens, width), t) for t in out_types],
        scratch_shapes=[pltpu.VMEM((tokens * len(rows), width), jnp.float32)],
        cost_estimate=pl.CostEstimate(
            flops=12 * tokens * len(rows) * width * hidden,
            bytes_accessed=12 * width * hidden,
            transcendentals=0,
        ),
        name="run_experts",
    )(who, *rows, *weights)


def gathered_body(
    queries,
    rotated_cache_keys,
    stored_cache_values,
    segment_new_keys,
    segment_new_values,
    block_ids,
    residual_in,
    out_weight,
    norm_gain,
    expert_ids,
    gate_scores,
    w_gate,
    w_up,
    w_down,
):
    parties = lax.axis_size("blk")
    deep, across = grid_of(parties)
    tokens = queries.shape[0]
    place = lax.axis_index("blk")
    my_deep = place // (across * CORES)
    my_across = place // CORES % across
    my_core = place % CORES
    groups = range(KEY_VALUE_HEADS)

    def moved(array, step_deep, step_across, step_core=0):
        return lax.ppermute(
            array, "blk", shift_pairs(deep, across, step_deep, step_across, step_core)
        )

    spots = [(dz, dx) for dz in range(deep) for dx in range(across)]
    order = [0] + [d for k in range(1, deep // 2 + 1) for d in sorted({k, deep - k})]
    sources = jnp.stack(
        [
            ((my_deep - dz) % deep * across + (my_across - dx) % across) * CORES + my_core
            for dz, dx in spots
        ]
    )

    def paired(keys, values, group):
        of = slice(group * HEAD_SIZE, (group + 1) * HEAD_SIZE)
        return jnp.concatenate([keys[:, of], values[:, of]], axis=1)

    blocks = {}
    for dz in order:
        for group in groups:
            if dz == 0:
                column = paired(rotated_cache_keys, stored_cache_values, group)
            elif dz <= deep // 2:
                column = moved(blocks[dz - 1, 0, group], 1, 0)
            else:
                column = moved(blocks[(dz + 1) % deep, 0, group], -1, 0)
            blocks[dz, 0, group] = column
            for dx in range(1, across):
                blocks[dz, dx, group] = moved(column, 0, dx)

    pair_queries = (queries, moved(queries, 0, 0, 1))
    chosen = jnp.concatenate(
        [
            jnp.tile(
                jnp.any(sources[:, None, None] == ids.T[None, :, :], axis=1).astype(jnp.float32),
                (1, TILE // tokens),
            )
            for ids in (block_ids, moved(block_ids, 0, 0, 1))
        ],
        axis=1,
    )
    weights = [w_gate, w_up, w_down]
    weights = weights + [moved(w, 0, 0, 1) for w in weights]
    who = jnp.stack([place, place + 1 - 2 * my_core])

    state = None
    for dz in order:
        for dx in range(across):
            pieces = [(g, dz * across + dx) for g in groups]
            given = [blocks[dz, dx, g] for g in groups]
            if state is None:
                pieces = [(g, None) for g in groups] + pieces
                given = [paired(segment_new_keys, segment_new_values, g) for g in groups] + given
            last = dz == order[-1] and dx == across - 1
            state = attend(pair_queries, chosen, state, pieces, given, last)

    mixing = gate_scores / jnp.sum(gate_scores, axis=1, keepdims=True)
    experts = jnp.arange(parties, dtype=jnp.int32)
    spread = jnp.sum(
        jnp.where(expert_ids[:, :, None] == experts[None, None, :], mixing[:, :, None], 0.0), axis=1
    )
    coarse = spread.astype(jnp.bfloat16)
    fine = (spread - coarse.astype(jnp.float32)).astype(jnp.bfloat16)
    extra = jnp.concatenate([coarse, fine], axis=1)
    extra = jnp.pad(extra, ((0, 0), (0, -extra.shape[1] % LANES)))

    near_stats, far_stats, near_out, far_out = state
    hidden_state, packed = pl.pallas_call(
        finish_kernel,
        out_shape=(
            jax.ShapeDtypeStruct(residual_in.shape, jnp.float32),
            jax.ShapeDtypeStruct((tokens, residual_in.shape[1] + extra.shape[1]), jnp.bfloat16),
        ),
        name="finish_attention",
    )(
        near_stats,
        near_out,
        moved(far_stats, 0, 0, 1),
        moved(far_out, 0, 0, 1),
        out_weight,
        residual_in,
        norm_gain.reshape(1, -1),
        extra,
    )

    rows = {(0, 0): packed}
    for dz in range(1, deep):
        rows[dz, 0] = moved(packed, dz, 0)
    for dz in range(deep):
        for dx in range(1, across):
            rows[dz, dx] = moved(rows[dz, 0], 0, dx)

    mixture = hidden_state
    for dz in order:
        results = run_experts(
            parties,
            who,
            [rows[dz, dx] for dx in range(across)],
            weights,
            [jnp.float32] + [jnp.bfloat16] * (across - 1),
        )
        column = results[0]
        for dx in range(1, across):
            column = column + moved(results[dx], 0, -dx).astype(jnp.float32)
        if dz:
            column = moved(column.astype(jnp.bfloat16), -dz, 0).astype(jnp.float32)
        mixture = mixture + column
    return mixture.astype(jnp.bfloat16)


def solution(mesh):
    placed = (
        P(("groups", "blk"), None),
        P(("groups", "blk"), None),
        P(("groups", "blk"), None),
        P(("groups", "blk"), None),
        P(("groups", "blk"), None),
        P(("groups", "blk"), None),
        P(("groups", "blk"), None),
        P(),
        P(),
        P(("groups", "blk"), None),
        P(("groups", "blk"), None),
        P("blk", None, None),
        P("blk", None, None),
        P("blk", None, None),
    )
    body = gathered_body if gathers(mesh) else routed_body
    return jax.shard_map(
        body, mesh=mesh, in_specs=placed, out_specs=P(("groups", "blk"), None), check_vma=False
    )
```

```python
import jax
import jax.numpy as jnp
from jax import lax
from jax.experimental import pallas as pl
from jax.experimental.pallas import tpu as pltpu
from jax.sharding import PartitionSpec as P


QUERY_HEADS = 16
KEY_VALUE_HEADS = 2
HEAD_SIZE = 128
TOPB = 8
TOPE = 8


NORM_EPSILON = 1e-06


def partials(query_rows, key_rows, value_rows, causal):
    queries_per_cluster = QUERY_HEADS // KEY_VALUE_HEADS
    score_scale = HEAD_SIZE ** (-0.5)
    maxima = []
    totals = []
    outputs = []
    for head_cluster in range(KEY_VALUE_HEADS):
        offset = head_cluster * queries_per_cluster * HEAD_SIZE
        group_queries = query_rows[:, offset : offset + queries_per_cluster * HEAD_SIZE].reshape(
            -1, HEAD_SIZE
        )
        group_keys = key_rows[:, head_cluster * HEAD_SIZE : (head_cluster + 1) * HEAD_SIZE]
        group_values = value_rows[:, head_cluster * HEAD_SIZE : (head_cluster + 1) * HEAD_SIZE]
        scores = (
            lax.dot_general(
                group_queries,
                group_keys,
                (((1,), (1,)), ((), ())),
                preferred_element_type=jnp.float32,
            )
            * score_scale
        )
        if causal:
            owner_row = jnp.arange(group_queries.shape[0], dtype=jnp.int32) // queries_per_cluster
            key_place = jnp.arange(key_rows.shape[0], dtype=jnp.int32)
            scores = jnp.where(key_place[None, :] <= owner_row[:, None], scores, -jnp.inf)
        row_max = jnp.max(scores, axis=1)
        weights = jnp.exp(scores - row_max[:, None])
        maxima.append(row_max.reshape(-1, queries_per_cluster))
        totals.append(jnp.sum(weights, axis=1).reshape(-1, queries_per_cluster))
        mixed_rows = jnp.dot(
            weights.astype(jnp.bfloat16), group_values, preferred_element_type=jnp.float32
        )
        outputs.append(mixed_rows.reshape(-1, queries_per_cluster * HEAD_SIZE))
    return (
        jnp.concatenate(maxima, axis=1),
        jnp.concatenate(totals, axis=1),
        jnp.concatenate(outputs, axis=1),
    )


def bucket_slots(targets, capacity, parties):
    flat_targets = targets.reshape(-1)
    pair_count = flat_targets.shape[0]
    one_hot = (flat_targets[:, None] == jnp.arange(parties, dtype=jnp.int32)[None, :]).astype(
        jnp.int32
    )
    before = jnp.sum((jnp.cumsum(one_hot, axis=0) - one_hot) * one_hot, axis=1)
    slot_index = flat_targets * capacity + before
    filler = (
        jnp.full((parties * capacity,), pair_count, jnp.int32)
        .at[slot_index]
        .set(jnp.arange(pair_count, dtype=jnp.int32))
    )
    return (slot_index, filler)


def routed_body(
    queries,
    rotated_cache_keys,
    stored_cache_values,
    segment_new_keys,
    segment_new_values,
    block_ids,
    residual_in,
    out_weight,
    norm_gain,
    expert_ids,
    gate_scores,
    w_gate,
    w_up,
    w_down,
):
    parties = lax.axis_size("blk")
    tok_count = queries.shape[0]
    capacity = tok_count * TOPB * 5 // (4 * parties)
    expert_capacity = tok_count * TOPE * 3 // (2 * parties)
    owner_slots, slot_pair = bucket_slots(block_ids, capacity, parties)
    pair_count = tok_count * TOPB
    occupied = slot_pair < pair_count
    source_token = jnp.minimum(slot_pair, pair_count - 1) // TOPB
    outgoing = jnp.where(
        occupied[:, None], queries[source_token], jnp.zeros((), queries.dtype)
    ).reshape(parties, capacity, QUERY_HEADS * HEAD_SIZE)
    arrived = lax.all_to_all(outgoing, "blk", split_axis=0, concat_axis=0, tiled=True)
    senders, items, row_width = arrived.shape
    far_max, far_total, far_out = partials(
        arrived.reshape(senders * items, row_width), rotated_cache_keys, stored_cache_values, False
    )
    back_max = lax.all_to_all(
        far_max.reshape(senders, items, QUERY_HEADS), "blk", split_axis=0, concat_axis=0, tiled=True
    )
    back_total = lax.all_to_all(
        far_total.reshape(senders, items, QUERY_HEADS),
        "blk",
        split_axis=0,
        concat_axis=0,
        tiled=True,
    )
    back_out = lax.all_to_all(
        far_out.astype(jnp.bfloat16).reshape(senders, items, row_width),
        "blk",
        split_axis=0,
        concat_axis=0,
        tiled=True,
    )
    local_row_maximum, local_denominator, local_output = partials(
        queries, segment_new_keys, segment_new_values, True
    )
    pair_max = back_max.reshape(-1, QUERY_HEADS)[owner_slots].reshape(tok_count, TOPB, QUERY_HEADS)
    pair_total = back_total.reshape(-1, QUERY_HEADS)[owner_slots].reshape(
        tok_count, TOPB, QUERY_HEADS
    )
    pair_out = back_out.reshape(-1, QUERY_HEADS * HEAD_SIZE)[owner_slots].reshape(
        tok_count, TOPB, QUERY_HEADS, HEAD_SIZE
    )
    ceiling = jnp.maximum(local_row_maximum, jnp.max(pair_max, axis=1))
    own_scale = jnp.exp(local_row_maximum - ceiling)
    pair_scale = jnp.exp(pair_max - ceiling[:, None, :])
    denominator = local_denominator * own_scale + jnp.sum(pair_total * pair_scale, axis=1)
    numerator = local_output.reshape(tok_count, QUERY_HEADS, HEAD_SIZE) * own_scale[
        :, :, None
    ] + jnp.einsum("tjh,tjhd->thd", pair_scale, pair_out, preferred_element_type=jnp.float32)
    attention = (
        (numerator / denominator[:, :, None])
        .reshape(tok_count, QUERY_HEADS * HEAD_SIZE)
        .astype(jnp.bfloat16)
    )
    hidden_state = residual_in.astype(jnp.float32) + jnp.dot(
        attention, out_weight, preferred_element_type=jnp.float32
    )
    normed = (
        hidden_state
        * lax.rsqrt(jnp.mean(hidden_state * hidden_state, axis=-1, keepdims=True) + NORM_EPSILON)
        * norm_gain
    ).astype(jnp.bfloat16)
    expert_slots, expert_pair = bucket_slots(expert_ids, expert_capacity, parties)
    expert_pairs = tok_count * TOPE
    expert_used = expert_pair < expert_pairs
    expert_token = jnp.minimum(expert_pair, expert_pairs - 1) // TOPE
    dispatched = jnp.where(
        expert_used[:, None], normed[expert_token], jnp.zeros((), normed.dtype)
    ).reshape(parties, expert_capacity, normed.shape[1])
    arrived = lax.all_to_all(dispatched, "blk", split_axis=0, concat_axis=0, tiled=True)
    flat_rows = arrived.reshape(-1, arrived.shape[2])
    gate_part = jnp.dot(flat_rows, w_gate[0], preferred_element_type=jnp.float32)
    up_part = jnp.dot(flat_rows, w_up[0], preferred_element_type=jnp.float32)
    inner = (jax.nn.silu(gate_part) * up_part).astype(jnp.bfloat16)
    expert_out = (
        jnp.dot(inner, w_down[0], preferred_element_type=jnp.float32)
        .astype(jnp.bfloat16)
        .reshape(arrived.shape)
    )
    returned = lax.all_to_all(expert_out, "blk", split_axis=0, concat_axis=0, tiled=True)
    gathered_rows = returned.reshape(-1, normed.shape[1])[expert_slots].reshape(
        tok_count, TOPE, normed.shape[1]
    )
    mixing = gate_scores / jnp.sum(gate_scores, axis=1, keepdims=True)
    mixture = jnp.einsum("tk,tkd->td", mixing, gathered_rows, preferred_element_type=jnp.float32)
    return (hidden_state + mixture).astype(jnp.bfloat16)


CORES = 2
LOG2_E = 1.4426950408889634
UNSEEN = -1e20
SKIPPED = 1e30
LANES = 128
TILE = 256
ONES_ROWS = 16
PIECE = 256
MIX_PIECE = 512
KERNEL_BYTES = 20 << 20


def grid_of(parties):
    chips = parties // CORES
    across = round(chips ** (1 / 3))
    while chips % across:
        across -= 1
    return (chips // across, across)


def visiting_order(deep):
    return [0] + [d for k in range(1, deep // 2 + 1) for d in sorted({k, deep - k})]


def gathers(mesh):
    return mesh.shape["blk"] <= 4 * TOPB and mesh.shape["blk"] % CORES == 0


def shift_pairs(deep, across, step_deep, step_across, step_core):
    return [
        (
            (z * across + x) * CORES + c,
            ((z + step_deep) % deep * across + (x + step_across) % across) * CORES
            + (c + step_core) % CORES,
        )
        for z in range(deep)
        for x in range(across)
        for c in range(CORES)
    ]


def attention_kernel(pieces, first, count, *refs):
    queries = refs[0:2]
    chosen_ref = refs[2]
    given = None if first else refs[3:7]
    block_refs = refs[-6 - count : -6]
    stats_refs = refs[-6:-4]
    out_refs = refs[-4:-2]
    score_refs = refs[-2:]
    tokens = queries[0].shape[0]
    per_tile = TILE // tokens
    heads_per_group = QUERY_HEADS // KEY_VALUE_HEADS
    factor = HEAD_SIZE ** (-0.5) * LOG2_E
    tasks = []
    for group in range(KEY_VALUE_HEADS):
        mine = []
        for (of_group, column), block_ref in zip(pieces, block_refs):
            if of_group == group:
                values = block_ref[:, HEAD_SIZE:].astype(jnp.float32).T.astype(jnp.bfloat16)
                ones = jnp.ones((ONES_ROWS, values.shape[1]), jnp.bfloat16)
                mine.append((column, block_ref, jnp.concatenate([values, ones], axis=0)))
        for owner in range(2):
            for tile in range(heads_per_group // per_tile):
                head = group * heads_per_group + tile * per_tile
                tasks += [
                    (owner, head, column, block_ref, mixer)
                    for column, block_ref, mixer in mine
                    if not (column is None and owner)
                ]

    def score(number):
        owner, head, column, block_ref, _ = tasks[number]
        rows = jnp.concatenate(
            [
                queries[owner][:, h * HEAD_SIZE : (h + 1) * HEAD_SIZE]
                for h in range(head, head + per_tile)
            ],
            axis=0,
        )
        keys = block_ref.shape[0]
        high = None
        for low in range(0, keys, PIECE):
            cut = slice(low, min(low + PIECE, keys))
            scores = lax.dot_general(
                block_ref[cut, :HEAD_SIZE],
                rows,
                (((1,), (1,)), ((), ())),
                preferred_element_type=jnp.float32,
            )
            if column is None:
                key = lax.broadcasted_iota(jnp.int32, scores.shape, 0) + low
                token = lax.broadcasted_iota(jnp.int32, scores.shape, 1) % tokens
                scores = jnp.where(key <= token, scores, -SKIPPED)
            score_refs[number % 2][cut, :] = scores
            part = jnp.max(scores, axis=0, keepdims=True)
            high = part if high is None else jnp.maximum(high, part)
        return high * factor

    seen = set()
    high = score(0)
    for number, (owner, head, column, block_ref, mixer) in enumerate(tasks):
        following = score(number + 1) if number + 1 < len(tasks) else None
        at = slice(head * tokens, head * tokens + TILE)
        if (owner, head) in seen:
            source = (stats_refs[owner], out_refs[owner])
        elif first:
            source = None
        else:
            source = (given[owner], given[2 + owner])
        seen.add((owner, head))
        top = source[0][0:1, at] if source else jnp.full((1, TILE), UNSEEN, jnp.float32)
        if column is None:
            high = jnp.maximum(top, high)
            shift = high
        else:
            chosen = chosen_ref[column : column + 1, owner * TILE : (owner + 1) * TILE] > 0.5
            high = jnp.maximum(top, jnp.where(chosen, high, UNSEEN))
            shift = jnp.where(chosen, high, SKIPPED)
        mixed = None
        keys = block_ref.shape[0]
        for low in range(0, keys, MIX_PIECE):
            cut = slice(low, min(low + MIX_PIECE, keys))
            scores = score_refs[number % 2][cut, :]
            weights = jnp.exp2(scores * factor - shift).astype(jnp.bfloat16)
            part = jnp.dot(mixer[:, cut], weights, preferred_element_type=jnp.float32)
            mixed = part if mixed is None else mixed + part
        out, total = mixed[:HEAD_SIZE], mixed[HEAD_SIZE : HEAD_SIZE + 1]
        if source:
            fade = jnp.exp2(top - high)
            out = source[1][:, at].astype(jnp.float32) * fade + out
            total = source[0][1:2, at] * fade + total
        stats_refs[owner][0:1, at] = high
        stats_refs[owner][1:2, at] = total
        out_refs[owner][:, at] = out.astype(out_refs[owner].dtype)
        high = following


def attend(queries, chosen, state, pieces, blocks, last=False):
    tokens = queries[0].shape[0]
    span = QUERY_HEADS * tokens
    stats = jax.ShapeDtypeStruct((8, span), jnp.float32)
    out = jax.ShapeDtypeStruct((HEAD_SIZE, span), jnp.float32)
    sent = jax.ShapeDtypeStruct((HEAD_SIZE, span), jnp.bfloat16)
    count = len(blocks)
    keys = sum(b.shape[0] for b in blocks)
    return pl.pallas_call(
        lambda *refs: attention_kernel(pieces, state is None, count, *refs),
        out_shape=(stats, stats, out, sent if last else out),
        scratch_shapes=[pltpu.VMEM((max(b.shape[0] for b in blocks), TILE), jnp.float32)] * 2,
        cost_estimate=pl.CostEstimate(
            flops=4 * keys * span * HEAD_SIZE,
            bytes_accessed=16 * HEAD_SIZE * span + keys * HEAD_SIZE * 4,
            transcendentals=keys * span,
        ),
        compiler_params=pltpu.CompilerParams(vmem_limit_bytes=KERNEL_BYTES),
        name="attend_blocks",
    )(*queries, chosen, *(state or ()), *blocks)


def finish_kernel(
    near_stats,
    near_out,
    far_stats,
    far_out,
    weight_ref,
    residual_ref,
    gain_ref,
    extra_ref,
    hidden_ref,
    packed_ref,
):
    tokens, width = residual_ref.shape
    near_top, far_top = near_stats[0:1, :], far_stats[0:1, :]
    ceiling = jnp.maximum(near_top, far_top)
    near_scale = jnp.exp2(near_top - ceiling)
    far_scale = jnp.exp2(far_top - ceiling)
    total = near_stats[1:2, :] * near_scale + far_stats[1:2, :] * far_scale
    mixed = near_out[...] * (near_scale / total) + far_out[...].astype(jnp.float32) * (
        far_scale / total
    )
    per_turn = LANES // tokens
    heads = []
    for turn in range(QUERY_HEADS // per_turn):
        turned = mixed[:, turn * LANES : (turn + 1) * LANES].T.astype(jnp.bfloat16)
        heads.extend(turned[n * tokens : (n + 1) * tokens] for n in range(per_turn))
    attention = jnp.concatenate(heads, axis=1)
    hidden = residual_ref[...].astype(jnp.float32) + jnp.dot(
        attention, weight_ref[...], preferred_element_type=jnp.float32
    )
    hidden_ref[...] = hidden
    mean = jnp.mean(hidden * hidden, axis=-1, keepdims=True)
    packed_ref[:, :width] = (hidden * lax.rsqrt(mean + NORM_EPSILON) * gain_ref[...]).astype(
        jnp.bfloat16
    )
    packed_ref[:, width:] = extra_ref[...]


def expert_kernel(parties, rows_count, *refs):
    who_ref = refs[0]
    row_refs = refs[1 : 1 + rows_count]
    weight_refs = refs[1 + rows_count : 7 + rows_count]
    out_refs = refs[7 + rows_count :]
    tokens, width = out_refs[0].shape
    block = jnp.concatenate([r[...] for r in row_refs], axis=0)
    inputs = block[:, :width]
    extra = block[:, width:].astype(jnp.float32)
    lane = lax.broadcasted_iota(jnp.int32, extra.shape, 1)
    result = None
    for slot in range(2):
        gate_ref, up_ref, down_ref = weight_refs[3 * slot : 3 * slot + 3]
        here = (lane == who_ref[slot]) | (lane == who_ref[slot] + parties)
        weight = jnp.sum(jnp.where(here, extra, 0.0), axis=1, keepdims=True)
        inner = []
        for low in range(0, gate_ref.shape[2], TILE):
            cut = slice(low, low + TILE)
            gate = jnp.dot(inputs, gate_ref[0, :, cut], preferred_element_type=jnp.float32)
            up = jnp.dot(inputs, up_ref[0, :, cut], preferred_element_type=jnp.float32)
            inner.append((gate / (1.0 + jnp.exp(-gate)) * up).astype(jnp.bfloat16))
        part = weight * jnp.dot(
            jnp.concatenate(inner, axis=1), down_ref[0], preferred_element_type=jnp.float32
        )
        result = part if result is None else result + part
    for n, out_ref in enumerate(out_refs):
        out_ref[...] = result[n * tokens : (n + 1) * tokens, :].astype(out_ref.dtype)


def run_experts(parties, who, rows, weights, out_types):
    tokens = rows[0].shape[0]
    _, width, hidden = weights[0].shape
    vmem = pl.BlockSpec(memory_space=pltpu.VMEM)
    return pl.pallas_call(
        lambda *refs: expert_kernel(parties, len(rows), *refs),
        in_specs=[pl.BlockSpec(memory_space=pltpu.SMEM)] + [vmem] * (len(rows) + len(weights)),
        out_shape=[jax.ShapeDtypeStruct((tokens, width), t) for t in out_types],
        cost_estimate=pl.CostEstimate(
            flops=12 * tokens * len(rows) * width * hidden,
            bytes_accessed=12 * width * hidden,
            transcendentals=0,
        ),
        compiler_params=pltpu.CompilerParams(vmem_limit_bytes=KERNEL_BYTES),
        name="run_experts",
    )(who, *rows, *weights)


def gathered_body(
    queries,
    rotated_cache_keys,
    stored_cache_values,
    segment_new_keys,
    segment_new_values,
    block_ids,
    residual_in,
    out_weight,
    norm_gain,
    expert_ids,
    gate_scores,
    w_gate,
    w_up,
    w_down,
):
    parties = lax.axis_size("blk")
    deep, across = grid_of(parties)
    tokens = queries.shape[0]
    place = lax.axis_index("blk")
    my_deep = place // (across * CORES)
    my_across = place // CORES % across
    my_core = place % CORES
    groups = range(KEY_VALUE_HEADS)

    def moved(array, step_deep, step_across, step_core=0):
        return lax.ppermute(
            array, "blk", shift_pairs(deep, across, step_deep, step_across, step_core)
        )

    spots = [(dz, dx) for dz in range(deep) for dx in range(across)]
    order = visiting_order(deep)
    sources = jnp.stack(
        [
            ((my_deep - dz) % deep * across + (my_across - dx) % across) * CORES + my_core
            for dz, dx in spots
        ]
    )

    def paired(keys, values, group):
        of = slice(group * HEAD_SIZE, (group + 1) * HEAD_SIZE)
        return jnp.concatenate([keys[:, of], values[:, of]], axis=1)

    blocks = {}
    for dz in order:
        for group in groups:
            if dz == 0:
                column = paired(rotated_cache_keys, stored_cache_values, group)
            elif dz <= deep // 2:
                column = moved(blocks[dz - 1, 0, group], 1, 0)
            else:
                column = moved(blocks[(dz + 1) % deep, 0, group], -1, 0)
            blocks[dz, 0, group] = column
            for dx in range(1, across):
                blocks[dz, dx, group] = moved(column, 0, dx)

    pair_queries = (queries, moved(queries, 0, 0, 1))
    chosen = jnp.concatenate(
        [
            jnp.tile(
                jnp.any(sources[:, None, None] == ids.T[None, :, :], axis=1).astype(jnp.float32),
                (1, TILE // tokens),
            )
            for ids in (block_ids, moved(block_ids, 0, 0, 1))
        ],
        axis=1,
    )
    weights = [w_gate, w_up, w_down]
    weights = weights + [moved(w, 0, 0, 1) for w in weights]
    who = jnp.stack([place, place + 1 - 2 * my_core])

    state = None
    for dz in order:
        for dx in range(across):
            pieces = [(g, dz * across + dx) for g in groups]
            given = [blocks[dz, dx, g] for g in groups]
            if state is None:
                pieces = [(g, None) for g in groups] + pieces
                given = [paired(segment_new_keys, segment_new_values, g) for g in groups] + given
            last = dz == order[-1] and dx == across - 1
            state = attend(pair_queries, chosen, state, pieces, given, last)

    mixing = gate_scores / jnp.sum(gate_scores, axis=1, keepdims=True)
    experts = jnp.arange(parties, dtype=jnp.int32)
    spread = jnp.sum(
        jnp.where(expert_ids[:, :, None] == experts[None, None, :], mixing[:, :, None], 0.0), axis=1
    )
    coarse = spread.astype(jnp.bfloat16)
    fine = (spread - coarse.astype(jnp.float32)).astype(jnp.bfloat16)
    extra = jnp.concatenate([coarse, fine], axis=1)
    extra = jnp.pad(extra, ((0, 0), (0, -extra.shape[1] % LANES)))

    near_stats, far_stats, near_out, far_out = state
    finish = pl.pallas_call(
        finish_kernel,
        out_shape=(
            jax.ShapeDtypeStruct(residual_in.shape, jnp.float32),
            jax.ShapeDtypeStruct((tokens, residual_in.shape[1] + extra.shape[1]), jnp.bfloat16),
        ),
        compiler_params=pltpu.CompilerParams(vmem_limit_bytes=KERNEL_BYTES),
        name="finish_attention",
    )
    arrived = (moved(far_stats, 0, 0, 1), moved(far_out, 0, 0, 1))
    hidden_state, packed = finish(
        near_stats, near_out, *arrived, out_weight, residual_in, norm_gain.reshape(1, -1), extra
    )

    rows = {(0, 0): packed}
    for dz in range(1, deep):
        rows[dz, 0] = moved(packed, dz, 0)
    for dz in range(deep):
        for dx in range(1, across):
            rows[dz, dx] = moved(rows[dz, 0], 0, dx)

    mixture = hidden_state
    for dz in order:
        results = run_experts(
            parties,
            who,
            [rows[dz, dx] for dx in range(across)],
            weights,
            [jnp.float32] + [jnp.bfloat16] * (across - 1),
        )
        column = results[0]
        for dx in range(1, across):
            column = column + moved(results[dx], 0, -dx).astype(jnp.float32)
        if dz:
            column = moved(column.astype(jnp.bfloat16), -dz, 0).astype(jnp.float32)
        mixture = mixture + column
    return mixture.astype(jnp.bfloat16)


def solution(mesh):
    placed = (
        P(("groups", "blk"), None),
        P(("groups", "blk"), None),
        P(("groups", "blk"), None),
        P(("groups", "blk"), None),
        P(("groups", "blk"), None),
        P(("groups", "blk"), None),
        P(("groups", "blk"), None),
        P(),
        P(),
        P(("groups", "blk"), None),
        P(("groups", "blk"), None),
        P("blk", None, None),
        P("blk", None, None),
        P("blk", None, None),
    )

    def shared(body):
        return jax.shard_map(
            body, mesh=mesh, in_specs=placed, out_specs=P(("groups", "blk"), None), check_vma=False
        )

    if not gathers(mesh):
        return shared(routed_body)

    return shared(gathered_body)
```

```python
import jax
import jax.numpy as jnp
from jax import lax
from jax.experimental import pallas as pl
from jax.experimental.pallas import tpu as pltpu
from jax.sharding import PartitionSpec as P


QUERY_HEADS = 16
KEY_VALUE_HEADS = 2
HEAD_SIZE = 128
TOPB = 8
TOPE = 8


NORM_EPSILON = 1e-06


def partials(query_rows, key_rows, value_rows, causal):
    queries_per_cluster = QUERY_HEADS // KEY_VALUE_HEADS
    score_scale = HEAD_SIZE ** (-0.5)
    maxima = []
    totals = []
    outputs = []
    for head_cluster in range(KEY_VALUE_HEADS):
        offset = head_cluster * queries_per_cluster * HEAD_SIZE
        group_queries = query_rows[:, offset : offset + queries_per_cluster * HEAD_SIZE].reshape(
            -1, HEAD_SIZE
        )
        group_keys = key_rows[:, head_cluster * HEAD_SIZE : (head_cluster + 1) * HEAD_SIZE]
        group_values = value_rows[:, head_cluster * HEAD_SIZE : (head_cluster + 1) * HEAD_SIZE]
        scores = (
            lax.dot_general(
                group_queries,
                group_keys,
                (((1,), (1,)), ((), ())),
                preferred_element_type=jnp.float32,
            )
            * score_scale
        )
        if causal:
            owner_row = jnp.arange(group_queries.shape[0], dtype=jnp.int32) // queries_per_cluster
            key_place = jnp.arange(key_rows.shape[0], dtype=jnp.int32)
            scores = jnp.where(key_place[None, :] <= owner_row[:, None], scores, -jnp.inf)
        row_max = jnp.max(scores, axis=1)
        weights = jnp.exp(scores - row_max[:, None])
        maxima.append(row_max.reshape(-1, queries_per_cluster))
        totals.append(jnp.sum(weights, axis=1).reshape(-1, queries_per_cluster))
        mixed_rows = jnp.dot(
            weights.astype(jnp.bfloat16), group_values, preferred_element_type=jnp.float32
        )
        outputs.append(mixed_rows.reshape(-1, queries_per_cluster * HEAD_SIZE))
    return (
        jnp.concatenate(maxima, axis=1),
        jnp.concatenate(totals, axis=1),
        jnp.concatenate(outputs, axis=1),
    )


def bucket_slots(targets, capacity, parties):
    flat_targets = targets.reshape(-1)
    pair_count = flat_targets.shape[0]
    one_hot = (flat_targets[:, None] == jnp.arange(parties, dtype=jnp.int32)[None, :]).astype(
        jnp.int32
    )
    before = jnp.sum((jnp.cumsum(one_hot, axis=0) - one_hot) * one_hot, axis=1)
    slot_index = flat_targets * capacity + before
    filler = (
        jnp.full((parties * capacity,), pair_count, jnp.int32)
        .at[slot_index]
        .set(jnp.arange(pair_count, dtype=jnp.int32))
    )
    return (slot_index, filler)


def routed_body(
    queries,
    rotated_cache_keys,
    stored_cache_values,
    segment_new_keys,
    segment_new_values,
    block_ids,
    residual_in,
    out_weight,
    norm_gain,
    expert_ids,
    gate_scores,
    w_gate,
    w_up,
    w_down,
):
    parties = lax.axis_size("blk")
    tok_count = queries.shape[0]
    capacity = tok_count * TOPB * 5 // (4 * parties)
    expert_capacity = tok_count * TOPE * 3 // (2 * parties)
    owner_slots, slot_pair = bucket_slots(block_ids, capacity, parties)
    pair_count = tok_count * TOPB
    occupied = slot_pair < pair_count
    source_token = jnp.minimum(slot_pair, pair_count - 1) // TOPB
    outgoing = jnp.where(
        occupied[:, None], queries[source_token], jnp.zeros((), queries.dtype)
    ).reshape(parties, capacity, QUERY_HEADS * HEAD_SIZE)
    arrived = lax.all_to_all(outgoing, "blk", split_axis=0, concat_axis=0, tiled=True)
    senders, items, row_width = arrived.shape
    far_max, far_total, far_out = partials(
        arrived.reshape(senders * items, row_width), rotated_cache_keys, stored_cache_values, False
    )
    back_max = lax.all_to_all(
        far_max.reshape(senders, items, QUERY_HEADS), "blk", split_axis=0, concat_axis=0, tiled=True
    )
    back_total = lax.all_to_all(
        far_total.reshape(senders, items, QUERY_HEADS),
        "blk",
        split_axis=0,
        concat_axis=0,
        tiled=True,
    )
    back_out = lax.all_to_all(
        far_out.astype(jnp.bfloat16).reshape(senders, items, row_width),
        "blk",
        split_axis=0,
        concat_axis=0,
        tiled=True,
    )
    local_row_maximum, local_denominator, local_output = partials(
        queries, segment_new_keys, segment_new_values, True
    )
    pair_max = back_max.reshape(-1, QUERY_HEADS)[owner_slots].reshape(tok_count, TOPB, QUERY_HEADS)
    pair_total = back_total.reshape(-1, QUERY_HEADS)[owner_slots].reshape(
        tok_count, TOPB, QUERY_HEADS
    )
    pair_out = back_out.reshape(-1, QUERY_HEADS * HEAD_SIZE)[owner_slots].reshape(
        tok_count, TOPB, QUERY_HEADS, HEAD_SIZE
    )
    ceiling = jnp.maximum(local_row_maximum, jnp.max(pair_max, axis=1))
    own_scale = jnp.exp(local_row_maximum - ceiling)
    pair_scale = jnp.exp(pair_max - ceiling[:, None, :])
    denominator = local_denominator * own_scale + jnp.sum(pair_total * pair_scale, axis=1)
    numerator = local_output.reshape(tok_count, QUERY_HEADS, HEAD_SIZE) * own_scale[
        :, :, None
    ] + jnp.einsum("tjh,tjhd->thd", pair_scale, pair_out, preferred_element_type=jnp.float32)
    attention = (
        (numerator / denominator[:, :, None])
        .reshape(tok_count, QUERY_HEADS * HEAD_SIZE)
        .astype(jnp.bfloat16)
    )
    hidden_state = residual_in.astype(jnp.float32) + jnp.dot(
        attention, out_weight, preferred_element_type=jnp.float32
    )
    normed = (
        hidden_state
        * lax.rsqrt(jnp.mean(hidden_state * hidden_state, axis=-1, keepdims=True) + NORM_EPSILON)
        * norm_gain
    ).astype(jnp.bfloat16)
    expert_slots, expert_pair = bucket_slots(expert_ids, expert_capacity, parties)
    expert_pairs = tok_count * TOPE
    expert_used = expert_pair < expert_pairs
    expert_token = jnp.minimum(expert_pair, expert_pairs - 1) // TOPE
    dispatched = jnp.where(
        expert_used[:, None], normed[expert_token], jnp.zeros((), normed.dtype)
    ).reshape(parties, expert_capacity, normed.shape[1])
    arrived = lax.all_to_all(dispatched, "blk", split_axis=0, concat_axis=0, tiled=True)
    flat_rows = arrived.reshape(-1, arrived.shape[2])
    gate_part = jnp.dot(flat_rows, w_gate[0], preferred_element_type=jnp.float32)
    up_part = jnp.dot(flat_rows, w_up[0], preferred_element_type=jnp.float32)
    inner = (jax.nn.silu(gate_part) * up_part).astype(jnp.bfloat16)
    expert_out = (
        jnp.dot(inner, w_down[0], preferred_element_type=jnp.float32)
        .astype(jnp.bfloat16)
        .reshape(arrived.shape)
    )
    returned = lax.all_to_all(expert_out, "blk", split_axis=0, concat_axis=0, tiled=True)
    gathered_rows = returned.reshape(-1, normed.shape[1])[expert_slots].reshape(
        tok_count, TOPE, normed.shape[1]
    )
    mixing = gate_scores / jnp.sum(gate_scores, axis=1, keepdims=True)
    mixture = jnp.einsum("tk,tkd->td", mixing, gathered_rows, preferred_element_type=jnp.float32)
    return (hidden_state + mixture).astype(jnp.bfloat16)


CORES = 2
LOG2_E = 1.4426950408889634
UNSEEN = -1e20
SKIPPED = 1e30
LANES = 128
TILE = 256
ONES_ROWS = 16
PARTS = 4
WEIGHT_PARTS = 8
PIECE = 256
KERNEL_BYTES = 20 << 20
ATTEND_BYTES = 10 << 20


def grid_of(parties):
    chips = parties // CORES
    across = round(chips ** (1 / 3))
    while chips % across:
        across -= 1
    return (chips // across, across)


def visiting_order(deep):
    return [0] + [d for k in range(1, deep // 2 + 1) for d in sorted({k, deep - k})]


def stages_of(deep, across):
    wide = range(1, across)
    later = [dz for dz in visiting_order(deep) if 1 < dz < deep - 1]
    stages = [[(0, 0)]] + [[(0, dx)] for dx in wide] + [[(1, 0)]] + [[(1, dx)] for dx in wide]
    stages += [[(dz, 0)] for dz in later] + [[(deep - 1, 0)]]
    stages += [[(dz, dx)] for dz in later + [deep - 1] for dx in wide]
    return [stage for stage in stages if stage]


def gathers(mesh):
    return mesh.shape["blk"] <= 4 * TOPB and mesh.shape["blk"] % CORES == 0


def shift_pairs(deep, across, step_deep, step_across, step_core):
    return [
        (
            (z * across + x) * CORES + c,
            ((z + step_deep) % deep * across + (x + step_across) % across) * CORES
            + (c + step_core) % CORES,
        )
        for z in range(deep)
        for x in range(across)
        for c in range(CORES)
    ]


def fetch(source, target, arrived, first, parts):
    rows = source.shape[-2] // parts
    copies = []
    for part in range(parts):
        cut = (*(slice(None),) * (len(source.shape) - 2), slice(part * rows, (part + 1) * rows))
        copies.append(
            pltpu.make_async_copy(source.at[cut], target.at[cut], arrived.at[first + part])
        )
        copies[-1].start()
    return copies


def attention_kernel(columns, first, *refs):
    count = len(columns)
    queries = refs[0:2]
    chosen_ref = refs[2]
    given = None if first else refs[3:7]
    inputs = 3 if first else 7
    sources = refs[inputs : inputs + 2 * count]
    results = refs[inputs + 2 * count :]
    stats_refs = results[0:2]
    out_refs = results[2:4]
    score_refs = results[4:6]
    held_ref, arrived = results[6:]
    copies = []
    held = []
    for number, source in enumerate(sources):
        held.append(held_ref.at[number, : source.shape[0], :])
        copies.append(fetch(source, held[-1], arrived, number * PARTS, PARTS))
    tokens = queries[0].shape[0]
    per_tile = TILE // tokens
    heads_per_group = QUERY_HEADS // KEY_VALUE_HEADS
    factor = HEAD_SIZE ** (-0.5) * LOG2_E
    tasks = [
        (owner, group * heads_per_group + tile * per_tile, group, number)
        for number in range(count)
        for group in range(KEY_VALUE_HEADS)
        for owner in range(1 if columns[number] is None else 2)
        for tile in range(heads_per_group // per_tile)
    ]
    mixers = {}

    def score(index):
        owner, head, group, number = tasks[index]
        of = slice(group * HEAD_SIZE, (group + 1) * HEAD_SIZE)
        if (number, group) not in mixers:
            if not group:
                for copy in copies[2 * number]:
                    copy.wait()
            mixers[number, group] = None
        rows = jnp.concatenate(
            [
                queries[owner][:, h * HEAD_SIZE : (h + 1) * HEAD_SIZE]
                for h in range(head, head + per_tile)
            ],
            axis=0,
        )
        keys = held[2 * number].shape[0]
        high = None
        for low in range(0, keys, PIECE):
            cut = slice(low, min(low + PIECE, keys))
            scores = lax.dot_general(
                held[2 * number][cut, of],
                rows,
                (((1,), (1,)), ((), ())),
                preferred_element_type=jnp.float32,
            )
            if columns[number] is None:
                key = lax.broadcasted_iota(jnp.int32, scores.shape, 0) + low
                token = lax.broadcasted_iota(jnp.int32, scores.shape, 1) % tokens
                scores = jnp.where(key <= token, scores, -SKIPPED)
            score_refs[index % 2][cut, :] = scores
            part = jnp.max(scores, axis=0, keepdims=True)
            high = part if high is None else jnp.maximum(high, part)
        return high * factor

    seen = set()
    high = score(0)
    for index, (owner, head, group, number) in enumerate(tasks):
        following = score(index + 1) if index + 1 < len(tasks) else None
        at = slice(head * tokens, head * tokens + TILE)
        if (owner, head) in seen:
            source = (stats_refs[owner], out_refs[owner])
        elif first:
            source = None
        else:
            source = (given[owner], given[2 + owner])
        seen.add((owner, head))
        top = source[0][0:1, at] if source else jnp.full((1, TILE), UNSEEN, jnp.float32)
        column = columns[number]
        if column is None:
            high = jnp.maximum(top, high)
            shift = high
        else:
            chosen = chosen_ref[column : column + 1, owner * TILE : (owner + 1) * TILE] > 0.5
            high = jnp.maximum(top, jnp.where(chosen, high, UNSEEN))
            shift = jnp.where(chosen, high, SKIPPED)
        if mixers[number, group] is None:
            if not group:
                for copy in copies[2 * number + 1]:
                    copy.wait()
            of = slice(group * HEAD_SIZE, (group + 1) * HEAD_SIZE)
            values = held[2 * number + 1][:, of].astype(jnp.float32).T.astype(jnp.bfloat16)
            ones = jnp.ones((ONES_ROWS, values.shape[1]), jnp.bfloat16)
            mixers[number, group] = jnp.concatenate([values, ones], axis=0)
        scores = score_refs[index % 2][: held[2 * number].shape[0], :]
        weights = jnp.exp2(scores * factor - shift).astype(jnp.bfloat16)
        mixed = jnp.dot(mixers[number, group], weights, preferred_element_type=jnp.float32)
        out, total = mixed[:HEAD_SIZE], mixed[HEAD_SIZE : HEAD_SIZE + 1]
        if source:
            fade = jnp.exp2(top - high)
            out = source[1][:, at].astype(jnp.float32) * fade + out
            total = source[0][1:2, at] * fade + total
        stats_refs[owner][0:1, at] = high
        stats_refs[owner][1:2, at] = total
        out_refs[owner][:, at] = out.astype(out_refs[owner].dtype)
        high = following


def attend(queries, chosen, state, columns, blocks, last=False):
    tokens = queries[0].shape[0]
    span = QUERY_HEADS * tokens
    stats = jax.ShapeDtypeStruct((8, span), jnp.float32)
    out = jax.ShapeDtypeStruct((HEAD_SIZE, span), jnp.float32)
    sent = jax.ShapeDtypeStruct((HEAD_SIZE, span), jnp.bfloat16)
    count = len(blocks)
    keys = sum(b.shape[0] for b in blocks) // 2
    longest = max(b.shape[0] for b in blocks)
    here = pl.BlockSpec(memory_space=pltpu.HBM)
    aliases = {3: 0, 4: 1, 5: 2} | ({} if last else {6: 3}) if state else {}
    return pl.pallas_call(
        lambda *refs: attention_kernel(columns, state is None, *refs),
        out_shape=(stats, stats, out, sent if last else out),
        input_output_aliases=aliases,
        in_specs=[pl.BlockSpec()] * (3 + len(state or ()))
        + [here] * count,
        scratch_shapes=[pltpu.VMEM((longest, TILE), jnp.float32)] * 2
        + [
            pltpu.VMEM((count, longest, blocks[0].shape[1]), jnp.bfloat16),
            pltpu.SemaphoreType.DMA((count * PARTS,)),
        ],
        cost_estimate=pl.CostEstimate(
            flops=8 * keys * span * HEAD_SIZE,
            bytes_accessed=16 * HEAD_SIZE * span + keys * HEAD_SIZE * 8,
            transcendentals=2 * keys * span,
        ),
        compiler_params=pltpu.CompilerParams(vmem_limit_bytes=ATTEND_BYTES),
        name="attend_blocks",
    )(*queries, chosen, *(state or ()), *blocks)


def finish_kernel(
    near_stats,
    near_out,
    far_stats,
    far_out,
    weight_ref,
    residual_ref,
    gain_ref,
    extra_ref,
    *refs,
):
    hidden_ref, packed_ref = refs[-2:]
    tokens, width = residual_ref.shape
    near_top, far_top = near_stats[0:1, :], far_stats[0:1, :]
    ceiling = jnp.maximum(near_top, far_top)
    near_scale = jnp.exp2(near_top - ceiling)
    far_scale = jnp.exp2(far_top - ceiling)
    total = near_stats[1:2, :] * near_scale + far_stats[1:2, :] * far_scale
    mixed = near_out[...] * (near_scale / total) + far_out[...].astype(jnp.float32) * (
        far_scale / total
    )
    per_turn = LANES // tokens
    heads = []
    for turn in range(QUERY_HEADS // per_turn):
        turned = mixed[:, turn * LANES : (turn + 1) * LANES].T.astype(jnp.bfloat16)
        heads.extend(turned[n * tokens : (n + 1) * tokens] for n in range(per_turn))
    attention = jnp.concatenate(heads, axis=1)
    hidden = residual_ref[...].astype(jnp.float32) + jnp.dot(
        attention, weight_ref[...], preferred_element_type=jnp.float32
    )
    hidden_ref[...] = hidden
    mean = jnp.mean(hidden * hidden, axis=-1, keepdims=True)
    packed_ref[:, :width] = (hidden * lax.rsqrt(mean + NORM_EPSILON) * gain_ref[...]).astype(
        jnp.bfloat16
    )
    packed_ref[:, width:] = extra_ref[...]


def expert_kernel(parties, rows_count, load, *refs):
    who_ref = refs[0]
    row_refs = refs[1 : 1 + rows_count]
    weight_refs = refs[1 + rows_count : 7 + rows_count]
    out_refs = refs[7 + rows_count : 7 + 2 * rows_count]
    copies = [[]] * 6
    if load:
        held_refs, arrived = refs[-7:-1], refs[-1]
        copies = [
            fetch(source, held_ref, arrived, number * WEIGHT_PARTS, WEIGHT_PARTS)
            for number, (source, held_ref) in enumerate(zip(weight_refs, held_refs))
        ]
        weight_refs = held_refs
    tokens, width = out_refs[0].shape
    block = jnp.concatenate([r[...] for r in row_refs], axis=0)
    inputs = block[:, :width]
    extra = block[:, width:].astype(jnp.float32)
    lane = lax.broadcasted_iota(jnp.int32, extra.shape, 1)
    result = None
    for slot in range(2):
        gate_ref, up_ref, down_ref = weight_refs[3 * slot : 3 * slot + 3]
        here = (lane == who_ref[slot]) | (lane == who_ref[slot] + parties)
        weight = jnp.sum(jnp.where(here, extra, 0.0), axis=1, keepdims=True)
        inner = []
        for copy in copies[3 * slot] + copies[3 * slot + 1]:
            copy.wait()
        for low in range(0, gate_ref.shape[2], TILE):
            cut = slice(low, low + TILE)
            gate = jnp.dot(inputs, gate_ref[0, :, cut], preferred_element_type=jnp.float32)
            up = jnp.dot(inputs, up_ref[0, :, cut], preferred_element_type=jnp.float32)
            inner.append((gate / (1.0 + jnp.exp(-gate)) * up).astype(jnp.bfloat16))
        for copy in copies[3 * slot + 2]:
            copy.wait()
        part = weight * jnp.dot(
            jnp.concatenate(inner, axis=1), down_ref[0], preferred_element_type=jnp.float32
        )
        result = part if result is None else result + part
    for n, out_ref in enumerate(out_refs):
        out_ref[...] = result[n * tokens : (n + 1) * tokens, :].astype(out_ref.dtype)


def run_experts(parties, who, rows, weights, out_types, load=False):
    tokens = rows[0].shape[0]
    _, width, hidden = weights[0].shape
    held = [jax.ShapeDtypeStruct(w.shape, w.dtype) for w in weights] if load else []
    return pl.pallas_call(
        lambda *refs: expert_kernel(parties, len(rows), load, *refs),
        in_specs=[pl.BlockSpec(memory_space=pltpu.SMEM)]
        + [pl.BlockSpec()] * len(rows)
        + [pl.BlockSpec(memory_space=pltpu.HBM) if load else pl.BlockSpec()] * len(weights),
        out_shape=[jax.ShapeDtypeStruct((tokens, width), t) for t in out_types] + held,
        scratch_shapes=[pltpu.SemaphoreType.DMA((len(weights) * WEIGHT_PARTS,))] if load else [],
        cost_estimate=pl.CostEstimate(
            flops=12 * tokens * len(rows) * width * hidden,
            bytes_accessed=12 * width * hidden,
            transcendentals=0,
        ),
        compiler_params=pltpu.CompilerParams(vmem_limit_bytes=KERNEL_BYTES),
        name="run_experts",
    )(who, *rows, *weights)


def gathered_body(
    queries,
    rotated_cache_keys,
    stored_cache_values,
    segment_new_keys,
    segment_new_values,
    block_ids,
    residual_in,
    out_weight,
    norm_gain,
    expert_ids,
    gate_scores,
    w_gate,
    w_up,
    w_down,
):
    parties = lax.axis_size("blk")
    deep, across = grid_of(parties)
    tokens = queries.shape[0]
    place = lax.axis_index("blk")
    my_deep = place // (across * CORES)
    my_across = place // CORES % across
    my_core = place % CORES

    def moved(array, step_deep, step_across, step_core=0):
        return lax.ppermute(
            array, "blk", shift_pairs(deep, across, step_deep, step_across, step_core)
        )

    spots = [(dz, dx) for dz in range(deep) for dx in range(across)]
    order = visiting_order(deep)
    sources = jnp.stack(
        [
            ((my_deep - dz) % deep * across + (my_across - dx) % across) * CORES + my_core
            for dz, dx in spots
        ]
    )

    blocks = {}
    for part, array in (("k", rotated_cache_keys), ("v", stored_cache_values)):
        for dz in order:
            if dz == 0:
                column = array
            elif dz <= deep // 2:
                column = moved(blocks[dz - 1, 0, part], 1, 0)
            else:
                column = moved(blocks[(dz + 1) % deep, 0, part], -1, 0)
            blocks[dz, 0, part] = column
            for dx in range(1, across):
                if part == "v" and dz == deep - 1:
                    blocks[dz, dx, part] = moved(blocks[0, dx, part], -1, 0)
                else:
                    blocks[dz, dx, part] = moved(column, 0, dx)

    pair_queries = (queries, moved(queries, 0, 0, 1))
    chosen = jnp.concatenate(
        [
            jnp.tile(
                jnp.any(sources[:, None, None] == ids.T[None, :, :], axis=1).astype(jnp.float32),
                (1, TILE // tokens),
            )
            for ids in (block_ids, moved(block_ids, 0, 0, 1))
        ],
        axis=1,
    )
    weights = [w_gate, w_up, w_down]
    weights = weights + [moved(w, 0, 0, 1) for w in weights]
    who = jnp.stack([place, place + 1 - 2 * my_core])

    state = None
    stages = stages_of(deep, across)
    for number, stage in enumerate(stages):
        columns = [dz * across + dx for dz, dx in stage]
        given = [blocks[dz, dx, part] for dz, dx in stage for part in "kv"]
        if state is None:
            columns = [None] + columns
            given = [segment_new_keys, segment_new_values] + given
        last = number == len(stages) - 1
        state = attend(pair_queries, chosen, state, columns, given, last)

    mixing = gate_scores / jnp.sum(gate_scores, axis=1, keepdims=True)
    experts = jnp.arange(parties, dtype=jnp.int32)
    spread = jnp.sum(
        jnp.where(expert_ids[:, :, None] == experts[None, None, :], mixing[:, :, None], 0.0), axis=1
    )
    coarse = spread.astype(jnp.bfloat16)
    fine = (spread - coarse.astype(jnp.float32)).astype(jnp.bfloat16)
    extra = jnp.concatenate([coarse, fine], axis=1)
    extra = jnp.pad(extra, ((0, 0), (0, -extra.shape[1] % LANES)))

    near_stats, far_stats, near_out, far_out = state
    finish = pl.pallas_call(
        finish_kernel,
        out_shape=(
            jax.ShapeDtypeStruct(residual_in.shape, jnp.float32),
            jax.ShapeDtypeStruct((tokens, residual_in.shape[1] + extra.shape[1]), jnp.bfloat16),
        ),
        compiler_params=pltpu.CompilerParams(vmem_limit_bytes=KERNEL_BYTES),
        name="finish_attention",
    )
    arrived = (moved(far_stats, 0, 0, 1), moved(far_out, 0, 0, 1))
    gain = norm_gain.reshape(1, -1)
    hidden_state, packed = finish(
        near_stats, near_out, *arrived, out_weight, residual_in, gain, extra
    )

    rows = {(0, 0): packed}
    for dz in range(1, deep):
        rows[dz, 0] = moved(packed, dz, 0)
    for dz in range(deep):
        for dx in range(1, across):
            rows[dz, dx] = moved(rows[dz, 0], 0, dx)

    wide = range(1, across)
    column, *on_chip = run_experts(parties, who, [packed], weights, [jnp.float32], True)
    mixture = hidden_state + column
    beside = [(0, dx) for dx in wide]
    for dz in [d for d in order if 1 < d < deep - 1] + [1, deep - 1]:
        direct = dz == deep - 1
        spots_now = [(dz, dx) for dx in range(across)] + beside
        results = run_experts(
            parties,
            who,
            [rows[spot] for spot in spots_now],
            on_chip,
            [jnp.bfloat16 if direct else jnp.float32]
            + [jnp.bfloat16] * (len(spots_now) - 1),
        )
        for n, (_, dx) in enumerate(beside):
            mixture = mixture + moved(results[across + n], 0, -dx).astype(jnp.float32)
        beside = []
        if direct:
            for dx in range(across):
                mixture = mixture + moved(results[dx], -dz, -dx).astype(jnp.float32)
            continue
        column = results[0]
        for dx in wide:
            column = column + moved(results[dx], 0, -dx).astype(jnp.float32)
        mixture = mixture + moved(column.astype(jnp.bfloat16), -dz, 0).astype(jnp.float32)
    return mixture.astype(jnp.bfloat16)


def solution(mesh):
    placed = (
        P(("groups", "blk"), None),
        P(("groups", "blk"), None),
        P(("groups", "blk"), None),
        P(("groups", "blk"), None),
        P(("groups", "blk"), None),
        P(("groups", "blk"), None),
        P(("groups", "blk"), None),
        P(),
        P(),
        P(("groups", "blk"), None),
        P(("groups", "blk"), None),
        P("blk", None, None),
        P("blk", None, None),
        P("blk", None, None),
    )

    def shared(body):
        return jax.shard_map(
            body, mesh=mesh, in_specs=placed, out_specs=P(("groups", "blk"), None), check_vma=False
        )

    if not gathers(mesh):
        return shared(routed_body)

    return shared(gathered_body)
```

```python
import jax
import jax.numpy as jnp
from jax import lax
from jax.experimental import pallas as pl
from jax.experimental.pallas import tpu as pltpu
from jax.sharding import PartitionSpec as P


QUERY_HEADS = 16
KEY_VALUE_HEADS = 2
HEAD_SIZE = 128
TOPB = 8
TOPE = 8


NORM_EPSILON = 1e-06


def partials(query_rows, key_rows, value_rows, causal):
    queries_per_cluster = QUERY_HEADS // KEY_VALUE_HEADS
    score_scale = HEAD_SIZE ** (-0.5)
    maxima = []
    totals = []
    outputs = []
    for head_cluster in range(KEY_VALUE_HEADS):
        offset = head_cluster * queries_per_cluster * HEAD_SIZE
        group_queries = query_rows[:, offset : offset + queries_per_cluster * HEAD_SIZE].reshape(
            -1, HEAD_SIZE
        )
        group_keys = key_rows[:, head_cluster * HEAD_SIZE : (head_cluster + 1) * HEAD_SIZE]
        group_values = value_rows[:, head_cluster * HEAD_SIZE : (head_cluster + 1) * HEAD_SIZE]
        scores = (
            lax.dot_general(
                group_queries,
                group_keys,
                (((1,), (1,)), ((), ())),
                preferred_element_type=jnp.float32,
            )
            * score_scale
        )
        if causal:
            owner_row = jnp.arange(group_queries.shape[0], dtype=jnp.int32) // queries_per_cluster
            key_place = jnp.arange(key_rows.shape[0], dtype=jnp.int32)
            scores = jnp.where(key_place[None, :] <= owner_row[:, None], scores, -jnp.inf)
        row_max = jnp.max(scores, axis=1)
        weights = jnp.exp(scores - row_max[:, None])
        maxima.append(row_max.reshape(-1, queries_per_cluster))
        totals.append(jnp.sum(weights, axis=1).reshape(-1, queries_per_cluster))
        mixed_rows = jnp.dot(
            weights.astype(jnp.bfloat16), group_values, preferred_element_type=jnp.float32
        )
        outputs.append(mixed_rows.reshape(-1, queries_per_cluster * HEAD_SIZE))
    return (
        jnp.concatenate(maxima, axis=1),
        jnp.concatenate(totals, axis=1),
        jnp.concatenate(outputs, axis=1),
    )


def bucket_slots(targets, capacity, parties):
    flat_targets = targets.reshape(-1)
    pair_count = flat_targets.shape[0]
    one_hot = (flat_targets[:, None] == jnp.arange(parties, dtype=jnp.int32)[None, :]).astype(
        jnp.int32
    )
    before = jnp.sum((jnp.cumsum(one_hot, axis=0) - one_hot) * one_hot, axis=1)
    slot_index = flat_targets * capacity + before
    filler = (
        jnp.full((parties * capacity,), pair_count, jnp.int32)
        .at[slot_index]
        .set(jnp.arange(pair_count, dtype=jnp.int32))
    )
    return (slot_index, filler)


def routed_body(
    queries,
    rotated_cache_keys,
    stored_cache_values,
    segment_new_keys,
    segment_new_values,
    block_ids,
    residual_in,
    out_weight,
    norm_gain,
    expert_ids,
    gate_scores,
    w_gate,
    w_up,
    w_down,
):
    parties = lax.axis_size("blk")
    tok_count = queries.shape[0]
    capacity = tok_count * TOPB * 5 // (4 * parties)
    expert_capacity = tok_count * TOPE * 3 // (2 * parties)
    owner_slots, slot_pair = bucket_slots(block_ids, capacity, parties)
    pair_count = tok_count * TOPB
    occupied = slot_pair < pair_count
    source_token = jnp.minimum(slot_pair, pair_count - 1) // TOPB
    outgoing = jnp.where(
        occupied[:, None], queries[source_token], jnp.zeros((), queries.dtype)
    ).reshape(parties, capacity, QUERY_HEADS * HEAD_SIZE)
    arrived = lax.all_to_all(outgoing, "blk", split_axis=0, concat_axis=0, tiled=True)
    senders, items, row_width = arrived.shape
    far_max, far_total, far_out = partials(
        arrived.reshape(senders * items, row_width), rotated_cache_keys, stored_cache_values, False
    )
    back_max = lax.all_to_all(
        far_max.reshape(senders, items, QUERY_HEADS), "blk", split_axis=0, concat_axis=0, tiled=True
    )
    back_total = lax.all_to_all(
        far_total.reshape(senders, items, QUERY_HEADS),
        "blk",
        split_axis=0,
        concat_axis=0,
        tiled=True,
    )
    back_out = lax.all_to_all(
        far_out.astype(jnp.bfloat16).reshape(senders, items, row_width),
        "blk",
        split_axis=0,
        concat_axis=0,
        tiled=True,
    )
    local_row_maximum, local_denominator, local_output = partials(
        queries, segment_new_keys, segment_new_values, True
    )
    pair_max = back_max.reshape(-1, QUERY_HEADS)[owner_slots].reshape(tok_count, TOPB, QUERY_HEADS)
    pair_total = back_total.reshape(-1, QUERY_HEADS)[owner_slots].reshape(
        tok_count, TOPB, QUERY_HEADS
    )
    pair_out = back_out.reshape(-1, QUERY_HEADS * HEAD_SIZE)[owner_slots].reshape(
        tok_count, TOPB, QUERY_HEADS, HEAD_SIZE
    )
    ceiling = jnp.maximum(local_row_maximum, jnp.max(pair_max, axis=1))
    own_scale = jnp.exp(local_row_maximum - ceiling)
    pair_scale = jnp.exp(pair_max - ceiling[:, None, :])
    denominator = local_denominator * own_scale + jnp.sum(pair_total * pair_scale, axis=1)
    numerator = local_output.reshape(tok_count, QUERY_HEADS, HEAD_SIZE) * own_scale[
        :, :, None
    ] + jnp.einsum("tjh,tjhd->thd", pair_scale, pair_out, preferred_element_type=jnp.float32)
    attention = (
        (numerator / denominator[:, :, None])
        .reshape(tok_count, QUERY_HEADS * HEAD_SIZE)
        .astype(jnp.bfloat16)
    )
    hidden_state = residual_in.astype(jnp.float32) + jnp.dot(
        attention, out_weight, preferred_element_type=jnp.float32
    )
    normed = (
        hidden_state
        * lax.rsqrt(jnp.mean(hidden_state * hidden_state, axis=-1, keepdims=True) + NORM_EPSILON)
        * norm_gain
    ).astype(jnp.bfloat16)
    expert_slots, expert_pair = bucket_slots(expert_ids, expert_capacity, parties)
    expert_pairs = tok_count * TOPE
    expert_used = expert_pair < expert_pairs
    expert_token = jnp.minimum(expert_pair, expert_pairs - 1) // TOPE
    dispatched = jnp.where(
        expert_used[:, None], normed[expert_token], jnp.zeros((), normed.dtype)
    ).reshape(parties, expert_capacity, normed.shape[1])
    arrived = lax.all_to_all(dispatched, "blk", split_axis=0, concat_axis=0, tiled=True)
    flat_rows = arrived.reshape(-1, arrived.shape[2])
    gate_part = jnp.dot(flat_rows, w_gate[0], preferred_element_type=jnp.float32)
    up_part = jnp.dot(flat_rows, w_up[0], preferred_element_type=jnp.float32)
    inner = (jax.nn.silu(gate_part) * up_part).astype(jnp.bfloat16)
    expert_out = (
        jnp.dot(inner, w_down[0], preferred_element_type=jnp.float32)
        .astype(jnp.bfloat16)
        .reshape(arrived.shape)
    )
    returned = lax.all_to_all(expert_out, "blk", split_axis=0, concat_axis=0, tiled=True)
    gathered_rows = returned.reshape(-1, normed.shape[1])[expert_slots].reshape(
        tok_count, TOPE, normed.shape[1]
    )
    mixing = gate_scores / jnp.sum(gate_scores, axis=1, keepdims=True)
    mixture = jnp.einsum("tk,tkd->td", mixing, gathered_rows, preferred_element_type=jnp.float32)
    return (hidden_state + mixture).astype(jnp.bfloat16)


CORES = 2
LOG2_E = 1.4426950408889634
UNSEEN = -1e20
SKIPPED = 1e30
LANES = 128
TILE = 256
ONES_ROWS = 16
PARTS = 4
WEIGHT_PARTS = 8
PIECE = 256
KERNEL_BYTES = 20 << 20
ATTEND_BYTES = 10 << 20


def grid_of(parties):
    chips = parties // CORES
    across = round(chips ** (1 / 3))
    while chips % across:
        across -= 1
    return (chips // across, across)


def visiting_order(deep):
    return [0] + [d for k in range(1, deep // 2 + 1) for d in sorted({k, deep - k})]


def stages_of(deep, across):
    wide = range(1, across)
    later = [dz for dz in visiting_order(deep) if 1 < dz < deep - 1]
    stages = [[(0, 0)]] + [[(0, dx)] for dx in wide] + [[(1, 0)]] + [[(1, dx)] for dx in wide]
    stages += [[(dz, 0) for dz in later + [deep - 1]]]
    stages += [[(dz, dx) for dz in later + [deep - 1] for dx in wide]]
    return [stage for stage in stages if stage]


def gathers(mesh):
    return mesh.shape["blk"] <= 4 * TOPB and mesh.shape["blk"] % CORES == 0


def shift_pairs(deep, across, step_deep, step_across, step_core):
    return [
        (
            (z * across + x) * CORES + c,
            ((z + step_deep) % deep * across + (x + step_across) % across) * CORES
            + (c + step_core) % CORES,
        )
        for z in range(deep)
        for x in range(across)
        for c in range(CORES)
    ]


def fetch(source, target, arrived, first, parts):
    rows = source.shape[-2] // parts
    copies = []
    for part in range(parts):
        cut = (*(slice(None),) * (len(source.shape) - 2), slice(part * rows, (part + 1) * rows))
        copies.append(
            pltpu.make_async_copy(source.at[cut], target.at[cut], arrived.at[first + part])
        )
        copies[-1].start()
    return copies


def attention_kernel(columns, first, *refs):
    count = len(columns)
    queries = refs[0:2]
    chosen_ref = refs[2]
    given = None if first else refs[3:7]
    inputs = 3 if first else 7
    sources = refs[inputs : inputs + 2 * count]
    results = refs[inputs + 2 * count :]
    stats_refs = results[0:2]
    out_refs = results[2:4]
    score_refs = results[4:6]
    spare_ref, held_ref, arrived = results[6:]
    copies = []
    held = []
    for number, source in enumerate(sources):
        held.append(held_ref.at[number, : source.shape[0], :])
        copies.append(fetch(source, held[-1], arrived, number * PARTS, PARTS))
    tokens = queries[0].shape[0]
    per_tile = TILE // tokens
    heads_per_group = QUERY_HEADS // KEY_VALUE_HEADS
    factor = HEAD_SIZE ** (-0.5) * LOG2_E
    tasks = [
        (owner, group * heads_per_group + tile * per_tile, group, number)
        for number in range(count)
        for group in range(KEY_VALUE_HEADS)
        for owner in range(1 if columns[number] is None else 2)
        for tile in range(heads_per_group // per_tile)
    ]
    mixers = {}

    def score(index):
        owner, head, group, number = tasks[index]
        of = slice(group * HEAD_SIZE, (group + 1) * HEAD_SIZE)
        if (number, group) not in mixers:
            if not group:
                for copy in copies[2 * number]:
                    copy.wait()
            mixers[number, group] = None
        rows = jnp.concatenate(
            [
                queries[owner][:, h * HEAD_SIZE : (h + 1) * HEAD_SIZE]
                for h in range(head, head + per_tile)
            ],
            axis=0,
        )
        keys = held[2 * number].shape[0]
        high = None
        for low in range(0, keys, PIECE):
            cut = slice(low, min(low + PIECE, keys))
            scores = lax.dot_general(
                held[2 * number][cut, of],
                rows,
                (((1,), (1,)), ((), ())),
                preferred_element_type=jnp.float32,
            )
            if columns[number] is None:
                key = lax.broadcasted_iota(jnp.int32, scores.shape, 0) + low
                token = lax.broadcasted_iota(jnp.int32, scores.shape, 1) % tokens
                scores = jnp.where(key <= token, scores, -SKIPPED)
            score_refs[index % 2][cut, :] = scores
            part = jnp.max(scores, axis=0, keepdims=True)
            high = part if high is None else jnp.maximum(high, part)
        return high * factor

    final = {task[:2]: index for index, task in enumerate(tasks)}
    seen = set()
    high = score(0)
    for index, (owner, head, group, number) in enumerate(tasks):
        following = score(index + 1) if index + 1 < len(tasks) else None
        at = slice(head * tokens, head * tokens + TILE)
        out_ref = out_refs[owner]
        narrow = out_ref.dtype != jnp.float32
        if (owner, head) in seen:
            source = (stats_refs[owner], spare_ref if narrow else out_ref)
        elif first:
            source = None
        else:
            source = (given[owner], given[2 + owner])
        seen.add((owner, head))
        top = source[0][0:1, at] if source else jnp.full((1, TILE), UNSEEN, jnp.float32)
        column = columns[number]
        if column is None:
            high = jnp.maximum(top, high)
            shift = high
        else:
            chosen = chosen_ref[column : column + 1, owner * TILE : (owner + 1) * TILE] > 0.5
            high = jnp.maximum(top, jnp.where(chosen, high, UNSEEN))
            shift = jnp.where(chosen, high, SKIPPED)
        if mixers[number, group] is None:
            if not group:
                for copy in copies[2 * number + 1]:
                    copy.wait()
            of = slice(group * HEAD_SIZE, (group + 1) * HEAD_SIZE)
            values = held[2 * number + 1][:, of].astype(jnp.float32).T.astype(jnp.bfloat16)
            ones = jnp.ones((ONES_ROWS, values.shape[1]), jnp.bfloat16)
            mixers[number, group] = jnp.concatenate([values, ones], axis=0)
        scores = score_refs[index % 2][: held[2 * number].shape[0], :]
        weights = jnp.exp2(scores * factor - shift).astype(jnp.bfloat16)
        mixed = jnp.dot(mixers[number, group], weights, preferred_element_type=jnp.float32)
        out, total = mixed[:HEAD_SIZE], mixed[HEAD_SIZE : HEAD_SIZE + 1]
        if source:
            fade = jnp.exp2(top - high)
            out = source[1][:, at].astype(jnp.float32) * fade + out
            total = source[0][1:2, at] * fade + total
        stats_refs[owner][0:1, at] = high
        stats_refs[owner][1:2, at] = total
        if narrow and index < final[owner, head]:
            out_ref = spare_ref
        out_ref[:, at] = out.astype(out_ref.dtype)
        high = following


def attend(queries, chosen, state, columns, blocks, last=False):
    tokens = queries[0].shape[0]
    span = QUERY_HEADS * tokens
    stats = jax.ShapeDtypeStruct((8, span), jnp.float32)
    out = jax.ShapeDtypeStruct((HEAD_SIZE, span), jnp.float32)
    sent = jax.ShapeDtypeStruct((HEAD_SIZE, span), jnp.bfloat16)
    count = len(blocks)
    keys = sum(b.shape[0] for b in blocks) // 2
    longest = max(b.shape[0] for b in blocks)
    here = pl.BlockSpec(memory_space=pltpu.HBM)
    aliases = {3: 0, 4: 1, 5: 2} | ({} if last else {6: 3}) if state else {}
    return pl.pallas_call(
        lambda *refs: attention_kernel(columns, state is None, *refs),
        out_shape=(stats, stats, out, sent if last else out),
        input_output_aliases=aliases,
        in_specs=[pl.BlockSpec()] * (3 + len(state or ()))
        + [here] * count,
        scratch_shapes=[pltpu.VMEM((longest, TILE), jnp.float32)] * 2
        + [
            pltpu.VMEM((HEAD_SIZE, span if last else LANES), jnp.float32),
            pltpu.VMEM((count, longest, blocks[0].shape[1]), jnp.bfloat16),
            pltpu.SemaphoreType.DMA((count * PARTS,)),
        ],
        cost_estimate=pl.CostEstimate(
            flops=8 * keys * span * HEAD_SIZE,
            bytes_accessed=16 * HEAD_SIZE * span + keys * HEAD_SIZE * 8,
            transcendentals=2 * keys * span,
        ),
        compiler_params=pltpu.CompilerParams(vmem_limit_bytes=ATTEND_BYTES),
        name="attend_blocks",
    )(*queries, chosen, *(state or ()), *blocks)


def finish_kernel(
    near_stats,
    near_out,
    far_stats,
    far_out,
    weight_ref,
    residual_ref,
    gain_ref,
    extra_ref,
    *refs,
):
    hidden_ref, packed_ref = refs[-2:]
    tokens, width = residual_ref.shape
    near_top, far_top = near_stats[0:1, :], far_stats[0:1, :]
    ceiling = jnp.maximum(near_top, far_top)
    near_scale = jnp.exp2(near_top - ceiling)
    far_scale = jnp.exp2(far_top - ceiling)
    total = near_stats[1:2, :] * near_scale + far_stats[1:2, :] * far_scale
    mixed = near_out[...] * (near_scale / total) + far_out[...].astype(jnp.float32) * (
        far_scale / total
    )
    per_turn = LANES // tokens
    heads = []
    for turn in range(QUERY_HEADS // per_turn):
        turned = mixed[:, turn * LANES : (turn + 1) * LANES].T.astype(jnp.bfloat16)
        heads.extend(turned[n * tokens : (n + 1) * tokens] for n in range(per_turn))
    attention = jnp.concatenate(heads, axis=1)
    hidden = residual_ref[...].astype(jnp.float32) + jnp.dot(
        attention, weight_ref[...], preferred_element_type=jnp.float32
    )
    hidden_ref[...] = hidden
    mean = jnp.mean(hidden * hidden, axis=-1, keepdims=True)
    packed_ref[:, :width] = (hidden * lax.rsqrt(mean + NORM_EPSILON) * gain_ref[...]).astype(
        jnp.bfloat16
    )
    packed_ref[:, width:] = extra_ref[...]


def expert_kernel(parties, rows_count, load, *refs):
    who_ref = refs[0]
    row_refs = refs[1 : 1 + rows_count]
    weight_refs = refs[1 + rows_count : 7 + rows_count]
    out_refs = refs[7 + rows_count : 7 + 2 * rows_count]
    copies = [[]] * 6
    if load:
        held_refs, arrived = refs[-7:-1], refs[-1]
        copies = [
            fetch(source, held_ref, arrived, number * WEIGHT_PARTS, WEIGHT_PARTS)
            for number, (source, held_ref) in enumerate(zip(weight_refs, held_refs))
        ]
        weight_refs = held_refs
    tokens, width = out_refs[0].shape
    block = jnp.concatenate([r[...] for r in row_refs], axis=0)
    inputs = block[:, :width]
    extra = block[:, width:].astype(jnp.float32)
    lane = lax.broadcasted_iota(jnp.int32, extra.shape, 1)
    result = None
    for slot in range(2):
        gate_ref, up_ref, down_ref = weight_refs[3 * slot : 3 * slot + 3]
        here = (lane == who_ref[slot]) | (lane == who_ref[slot] + parties)
        weight = jnp.sum(jnp.where(here, extra, 0.0), axis=1, keepdims=True)
        inner = []
        for copy in copies[3 * slot] + copies[3 * slot + 1]:
            copy.wait()
        for low in range(0, gate_ref.shape[2], TILE):
            cut = slice(low, low + TILE)
            gate = jnp.dot(inputs, gate_ref[0, :, cut], preferred_element_type=jnp.float32)
            up = jnp.dot(inputs, up_ref[0, :, cut], preferred_element_type=jnp.float32)
            inner.append((gate / (1.0 + jnp.exp(-gate)) * up).astype(jnp.bfloat16))
        for copy in copies[3 * slot + 2]:
            copy.wait()
        part = weight * jnp.dot(
            jnp.concatenate(inner, axis=1), down_ref[0], preferred_element_type=jnp.float32
        )
        result = part if result is None else result + part
    for n, out_ref in enumerate(out_refs):
        out_ref[...] = result[n * tokens : (n + 1) * tokens, :].astype(out_ref.dtype)


def run_experts(parties, who, rows, weights, out_types, load=False):
    tokens = rows[0].shape[0]
    _, width, hidden = weights[0].shape
    held = [jax.ShapeDtypeStruct(w.shape, w.dtype) for w in weights] if load else []
    return pl.pallas_call(
        lambda *refs: expert_kernel(parties, len(rows), load, *refs),
        in_specs=[pl.BlockSpec(memory_space=pltpu.SMEM)]
        + [pl.BlockSpec()] * len(rows)
        + [pl.BlockSpec(memory_space=pltpu.HBM) if load else pl.BlockSpec()] * len(weights),
        out_shape=[jax.ShapeDtypeStruct((tokens, width), t) for t in out_types] + held,
        scratch_shapes=[pltpu.SemaphoreType.DMA((len(weights) * WEIGHT_PARTS,))] if load else [],
        cost_estimate=pl.CostEstimate(
            flops=12 * tokens * len(rows) * width * hidden,
            bytes_accessed=12 * width * hidden,
            transcendentals=0,
        ),
        compiler_params=pltpu.CompilerParams(vmem_limit_bytes=KERNEL_BYTES),
        name="run_experts",
    )(who, *rows, *weights)


def gathered_body(
    queries,
    rotated_cache_keys,
    stored_cache_values,
    segment_new_keys,
    segment_new_values,
    block_ids,
    residual_in,
    out_weight,
    norm_gain,
    expert_ids,
    gate_scores,
    w_gate,
    w_up,
    w_down,
):
    parties = lax.axis_size("blk")
    deep, across = grid_of(parties)
    tokens = queries.shape[0]
    place = lax.axis_index("blk")
    my_deep = place // (across * CORES)
    my_across = place // CORES % across
    my_core = place % CORES

    def moved(array, step_deep, step_across, step_core=0):
        return lax.ppermute(
            array, "blk", shift_pairs(deep, across, step_deep, step_across, step_core)
        )

    spots = [(dz, dx) for dz in range(deep) for dx in range(across)]
    order = visiting_order(deep)
    sources = jnp.stack(
        [
            ((my_deep - dz) % deep * across + (my_across - dx) % across) * CORES + my_core
            for dz, dx in spots
        ]
    )

    blocks = {}
    for part, array in (("k", rotated_cache_keys), ("v", stored_cache_values)):
        for dz in order:
            if dz == 0:
                column = array
            elif dz <= deep // 2:
                column = moved(blocks[dz - 1, 0, part], 1, 0)
            else:
                column = moved(blocks[(dz + 1) % deep, 0, part], -1, 0)
            blocks[dz, 0, part] = column
            for dx in range(1, across):
                if part == "v" and dz == deep - 1:
                    blocks[dz, dx, part] = moved(blocks[0, dx, part], -1, 0)
                else:
                    blocks[dz, dx, part] = moved(column, 0, dx)

    pair_queries = (queries, moved(queries, 0, 0, 1))
    chosen = jnp.concatenate(
        [
            jnp.tile(
                jnp.any(sources[:, None, None] == ids.T[None, :, :], axis=1).astype(jnp.float32),
                (1, TILE // tokens),
            )
            for ids in (block_ids, moved(block_ids, 0, 0, 1))
        ],
        axis=1,
    )
    weights = [w_gate, w_up, w_down]
    weights = weights + [moved(w, 0, 0, 1) for w in weights]
    who = jnp.stack([place, place + 1 - 2 * my_core])

    state = None
    stages = stages_of(deep, across)
    for number, stage in enumerate(stages):
        columns = [dz * across + dx for dz, dx in stage]
        given = [blocks[dz, dx, part] for dz, dx in stage for part in "kv"]
        if state is None:
            columns = [None] + columns
            given = [segment_new_keys, segment_new_values] + given
        last = number == len(stages) - 1
        state = attend(pair_queries, chosen, state, columns, given, last)

    mixing = gate_scores / jnp.sum(gate_scores, axis=1, keepdims=True)
    experts = jnp.arange(parties, dtype=jnp.int32)
    spread = jnp.sum(
        jnp.where(expert_ids[:, :, None] == experts[None, None, :], mixing[:, :, None], 0.0), axis=1
    )
    coarse = spread.astype(jnp.bfloat16)
    fine = (spread - coarse.astype(jnp.float32)).astype(jnp.bfloat16)
    extra = jnp.concatenate([coarse, fine], axis=1)
    extra = jnp.pad(extra, ((0, 0), (0, -extra.shape[1] % LANES)))

    near_stats, far_stats, near_out, far_out = state
    finish = pl.pallas_call(
        finish_kernel,
        out_shape=(
            jax.ShapeDtypeStruct(residual_in.shape, jnp.float32),
            jax.ShapeDtypeStruct((tokens, residual_in.shape[1] + extra.shape[1]), jnp.bfloat16),
        ),
        compiler_params=pltpu.CompilerParams(vmem_limit_bytes=KERNEL_BYTES),
        name="finish_attention",
    )
    arrived = (moved(far_stats, 0, 0, 1), moved(far_out, 0, 0, 1))
    gain = norm_gain.reshape(1, -1)
    hidden_state, packed = finish(
        near_stats, near_out, *arrived, out_weight, residual_in, gain, extra
    )

    rows = {(0, 0): packed}
    for dz in range(1, deep):
        rows[dz, 0] = moved(packed, dz, 0)
    for dz in range(deep):
        for dx in range(1, across):
            rows[dz, dx] = moved(rows[dz, 0], 0, dx)

    wide = range(1, across)
    column, *on_chip = run_experts(parties, who, [packed], weights, [jnp.float32], True)
    mixture = hidden_state + column
    beside = [(0, dx) for dx in wide]
    for dz in [d for d in order if 1 < d < deep - 1] + [1, deep - 1]:
        direct = dz == deep - 1
        spots_now = [(dz, dx) for dx in range(across)] + beside
        results = run_experts(
            parties,
            who,
            [rows[spot] for spot in spots_now],
            on_chip,
            [jnp.bfloat16 if direct else jnp.float32]
            + [jnp.bfloat16] * (len(spots_now) - 1),
        )
        for n, (_, dx) in enumerate(beside):
            mixture = mixture + moved(results[across + n], 0, -dx).astype(jnp.float32)
        beside = []
        if direct:
            for dx in range(across):
                mixture = mixture + moved(results[dx], -dz, -dx).astype(jnp.float32)
            continue
        column = results[0]
        for dx in wide:
            column = column + moved(results[dx], 0, -dx).astype(jnp.float32)
        mixture = mixture + moved(column.astype(jnp.bfloat16), -dz, 0).astype(jnp.float32)
    return mixture.astype(jnp.bfloat16)


def solution(mesh):
    placed = (
        P(("groups", "blk"), None),
        P(("groups", "blk"), None),
        P(("groups", "blk"), None),
        P(("groups", "blk"), None),
        P(("groups", "blk"), None),
        P(("groups", "blk"), None),
        P(("groups", "blk"), None),
        P(),
        P(),
        P(("groups", "blk"), None),
        P(("groups", "blk"), None),
        P("blk", None, None),
        P("blk", None, None),
        P("blk", None, None),
    )

    def shared(body):
        return jax.shard_map(
            body, mesh=mesh, in_specs=placed, out_specs=P(("groups", "blk"), None), check_vma=False
        )

    if not gathers(mesh):
        return shared(routed_body)

    return shared(gathered_body)
```
